128 devices in a mesh: dp: 4 (over x), expert: 32 (over z, y, core).
Axes of the slice: x: 4, y: 4, z: 4, core: 2. Of those that a mesh axis runs over, the one named last changes fastest.
Arguments:
- master: float32 [2, 128, 64, 2880], P(None, 'expert', 'dp'), may hold values from -6 to 6
- moment_one: float32 [2, 128, 64, 2880], P(None, 'expert', 'dp'), may hold values from -1.2 to 1.2
- moment_two: float32 [2, 128, 64, 2880], P(None, 'expert', 'dp'), may hold values from 0.0005 to 0.5
- gradient: bfloat16 [2, 128, 64, 2880], P(None, 'expert', 'dp'), may hold values from -150000 to 150000
- old_slot: int32 [2, 128], replicated, may hold values from 0 to 127, as said below
- new_slot: int32 [2, 128], replicated, may hold values from 0 to 127, as said below
Outputs:
- new_master: float32 [2, 128, 64, 2880], P(None, 'expert', 'dp')
- new_moment_one: float32 [2, 128, 64, 2880], P(None, 'expert', 'dp')
- new_moment_two: float32 [2, 128, 64, 2880], P(None, 'expert', 'dp')
The draws below stay inside these ranges and needn't reach their ends.
Inputs may be any that keep to these rules, and one draw needn't show every extreme that they name: `old_slot`: for each layer a permutation of 0 to 127; global slot s is held by index s // 4 of expert. `new_slot`: for each layer a permutation of 0 to 127; in each layer exactly 1 slot of each index of expert receives another expert than it held, and exactly 1 of the experts held by each index leaves its slot; all other experts keep their slot.
All inputs are finite; a program needn't handle non-finite values.
Results may differ from the reference program's by a relative error of at most 0.001.
Values sent between devices are 32-bit elements; how exact they have to be, the bound alone decides.
A program may use at most 64 MiB of HBM per device.

```python
import math
import jax
import jax.numpy as jnp
from jax import lax

D = 2880
EXP_DEV = 4
EXPERTS = 128
RROWS = 64
LAYERS = 2
MOVE_DEV = 1


def placement_pair(key):
    base_key = jax.random.fold_in(key, 17)
    group_size = EXPERTS // EXP_DEV
    old_tables = []
    new_tables = []
    for layer_index in range(LAYERS):
        layer_key = jax.random.fold_in(base_key, layer_index)
        key_perm, key_pick, key_cycle = jax.random.split(layer_key, 3)
        old_layer = jax.random.permutation(key_perm, EXPERTS).astype(jnp.int32)
        scores = jax.random.randint(key_pick, (group_size, EXP_DEV), 0, 1 << 20, dtype=jnp.int32) * EXP_DEV
        scores = scores + lax.broadcasted_iota(jnp.int32, (group_size, EXP_DEV), 1)
        chosen = jnp.argsort(scores, axis=1)[:, :MOVE_DEV].astype(jnp.int32)
        chosen = (chosen + lax.broadcasted_iota(jnp.int32, chosen.shape, 0) * EXP_DEV).reshape(-1)
        cycle_order = jax.random.permutation(key_cycle, group_size * MOVE_DEV).astype(jnp.int32)
        ordered = chosen[cycle_order]
        destination = jnp.arange(EXPERTS, dtype=jnp.int32).at[ordered].set(jnp.roll(ordered, -1))
        old_tables.append(old_layer)
        new_tables.append(destination[old_layer].astype(jnp.int32))
    return (jnp.stack(old_tables), jnp.stack(new_tables))


def draw_old_slot(key, part):
    return placement_pair(key)[0]


def draw_new_slot(key, part):
    return placement_pair(key)[1]


def draw_gradient(key, part):
    key_noise = jax.random.fold_in(jax.random.fold_in(key, 29), 0)
    key_row = jax.random.fold_in(jax.random.fold_in(key, 29), 1)
    key_col = jax.random.fold_in(jax.random.fold_in(key, 29), 2)
    key_block = jax.random.fold_in(jax.random.fold_in(key, 29), 4)
    key_total = jax.random.fold_in(jax.random.fold_in(key, 29), 5)
    full_shape = (LAYERS, EXPERTS, RROWS, D)
    slot_place = lax.broadcasted_iota(jnp.float32, (1, EXPERTS, 1, 1), 1) / (EXPERTS - 1)
    block_scale = jnp.exp(jax.random.uniform(key_block, (LAYERS, EXPERTS, 1, 1), jnp.float32, 0.0, math.log(2.0)))
    total_scale = jnp.exp(jax.random.uniform(key_total, (), jnp.float32, 0.0, math.log(4.0)))
    slot_rise = 1.0 + 2.0 * slot_place
    noise = jax.random.normal(key_noise, full_shape, jnp.float32)
    row_scale = jnp.exp(jax.random.uniform(key_row, (LAYERS, EXPERTS, RROWS, 1), jnp.float32, 0.0, math.log(10.0)))
    col_scale = jnp.exp(jax.random.uniform(key_col, (LAYERS, 1, 1, D), jnp.float32, 0.0, math.log(10.0)))
    return (noise * row_scale * col_scale * slot_rise * block_scale * total_scale).astype(jnp.bfloat16)


def steps_of(own_key, extent, cuts, smallest, high):
    def one(dim, shards_of):
        heights = jax.random.uniform(jax.random.fold_in(jax.random.fold_in(own_key, 6), dim), (shards_of,), jnp.float32, smallest / len(cuts), high / len(cuts))
        return jnp.repeat(jnp.exp(heights), extent[dim] // shards_of).reshape((-1,) + (1,) * (len(extent) - dim - 1))

    gain = one(*cuts[0])
    for cut in cuts[1:]:
        gain = gain * one(*cut)
    return gain


def gaussian(stream_key, dims, scale, reach, cuts=(), kind=jnp.bfloat16):
    array = scale * jax.random.normal(stream_key, dims, jnp.float32)
    if cuts:
        array = array * steps_of(stream_key, dims, cuts, -0.22, 0.18)
    return jnp.clip(array, -reach, reach).astype(kind)


def setup_inputs(seed: int = 0) -> dict:
    key_of = jax.random.split(jax.random.key(seed), 7)
    return {
        "master": gaussian(key_of[0], (LAYERS, EXPERTS, RROWS, D), 1.0, 6.0, ((1, 32), (2, 4)), jnp.float32),
        "moment_one": gaussian(key_of[1], (LAYERS, EXPERTS, RROWS, D), 0.2, 1.2, ((1, 32), (2, 4)), jnp.float32),
        "moment_two": jnp.clip(jnp.exp(math.log(0.5) - 6.9077552 * jax.random.uniform(key_of[2], (LAYERS, EXPERTS, RROWS, D), jnp.float32) ** steps_of(key_of[2], (LAYERS, EXPERTS, RROWS, D), ((1, 32), (2, 4)), -0.2, 0.2)), 0.0005, 0.5),
        "gradient": draw_gradient(jax.random.fold_in(key_of[6], 71), 0),
        "old_slot": draw_old_slot(jax.random.fold_in(key_of[6], 71), 0),
        "new_slot": draw_new_slot(jax.random.fold_in(key_of[6], 71), 0),
    }


BETA_ONE = 0.9
BETA_TWO = 0.95
LEARN_RATE = 0.05
DECAY_RATE = 0.1
ADAM_EPS = 1e-08
CLIP_RMS = 2.0
FIRST_FIX = 1.0 - 0.9 ** 10
SECOND_FIX = 1.0 - 0.95 ** 10

def adam_update(master, moment_one, moment_two, gradient, clip_scale):
    scaled = gradient.astype(jnp.float32) * clip_scale
    first_moment = BETA_ONE * moment_one + (1.0 - BETA_ONE) * scaled
    second = BETA_TWO * moment_two + (1.0 - BETA_TWO) * scaled * scaled
    step_dir = first_moment / FIRST_FIX / (jnp.sqrt(second / SECOND_FIX) + ADAM_EPS)
    weights = master - LEARN_RATE * (step_dir + DECAY_RATE * master)
    return (weights, first_moment, second)

def clip_factor(square_sum, entry_count):
    return jnp.minimum(1.0, CLIP_RMS * math.sqrt(entry_count) / (jnp.sqrt(square_sum) + 1e-06))

def pick_rows(data, chosen):
    return jax.vmap(lambda layer_block, layer_pick: jnp.take(layer_block, layer_pick, axis=0))(data, chosen)

def reference(master, moment_one, moment_two, gradient, old_slot, new_slot):
    widened = gradient.astype(jnp.float32)
    square_sum = jnp.sum(widened * widened)
    clip_scale = clip_factor(square_sum, LAYERS * EXPERTS * RROWS * D)
    updated = adam_update(master, moment_one, moment_two, gradient, clip_scale)
    holder = jnp.argsort(new_slot, axis=1).astype(jnp.int32)
    source = jnp.take_along_axis(old_slot, holder, axis=1).astype(jnp.int32)
    return (pick_rows(updated[0], source), pick_rows(updated[1], source), pick_rows(updated[2], source))
```

```python
import functools
import math

import jax
import jax.numpy as jnp
from jax import lax
from jax.experimental import pallas as pl
from jax.experimental.pallas import tpu as pltpu
from jax.sharding import PartitionSpec as P

BETA_ONE = 0.9
BETA_TWO = 0.95
LEARN_RATE = 0.05
DECAY_RATE = 0.1
ADAM_EPS = 1e-08
CLIP_RMS = 2.0
FIRST_FIX = 1.0 - 0.9**10
SECOND_FIX = 1.0 - 0.95**10

ZDIM, YDIM, CORES = 4, 4, 2
GROUP = ZDIM * YDIM * CORES
DP = 4
LANES = 128
SUB = 4
PIECE = 3
HOLDERS = 30


def move_order():
    moves = [
        (dz, dy, dc)
        for dz in (0, 1, 2, -1)
        for dy in (0, 1, 2, -1)
        for dc in (0, 1)
        if (dz, dy, dc) != (0, 0, 0)
    ]
    neg = lambda v: v if v == 2 else -v
    order = []
    for dz, dy, dc in sorted(moves, key=lambda m: -(abs(m[0]) + abs(m[1]))):
        for m in ((dz, dy, dc), (neg(dz), neg(dy), dc), (dy, dz, dc), (neg(dy), neg(dz), dc)):
            if m not in order:
                order.append(m)
    return order


MOVES = move_order()


def shifted(me, move, sign=1):
    dz, dy, dc = move
    core, y, z = me % CORES, (me // CORES) % YDIM, me // (CORES * YDIM)
    z = (z + sign * dz + ZDIM) % ZDIM
    y = (y + sign * dy + YDIM) % YDIM
    return (z * YDIM + y) * CORES + (core + dc) % CORES


def adam(master, moment_one, moment_two, gradient, scale):
    scaled = gradient * scale
    first = BETA_ONE * moment_one + (1.0 - BETA_ONE) * scaled
    second = BETA_TWO * moment_two + (1.0 - BETA_TWO) * scaled * scaled
    step = (first * (1.0 / FIRST_FIX)) / (jnp.sqrt(second * (1.0 / SECOND_FIX)) + ADAM_EPS)
    return master - LEARN_RATE * (step + DECAY_RATE * master), first, second


def exchange_kernel(
    entry_count,
    plan,
    master_hbm,
    one_hbm,
    two_hbm,
    grad_hbm,
    new_w,
    new_one,
    new_two,
    landed,
    master,
    one,
    two,
    grad,
    send_raw,
    send_new,
    hold_raw,
    hold_new,
    back_0,
    back_1,
    home,
    part,
    parts,
    line,
    lines,
    load_sem,
    part_send,
    part_recv,
    line_send,
    line_recv,
    out_send,
    out_recv,
    back_send,
    back_recv,
):
    layers, slots, rows, cols = master.shape
    full = cols // LANES
    dp = lax.axis_index("dp")
    me = lax.axis_index("expert")
    targets = [shifted(me, m) for m in MOVES]
    sources = [shifted(me, m, -1) for m in MOVES]

    loads = [
        pltpu.make_async_copy(src, dst, load_sem.at[i])
        for i, (src, dst) in enumerate(
            ((grad_hbm, grad), (master_hbm, master), (one_hbm, one), (two_hbm, two))
        )
    ]
    for load in loads:
        load.start()

    barrier = pltpu.get_barrier_semaphore()
    for t in targets:
        pl.semaphore_signal(barrier, inc=1, device_id={"expert": t})
    for d in range(1, DP):
        pl.semaphore_signal(barrier, inc=1, device_id={"dp": (dp + d) % DP})

    loads[0].wait()

    def square(i, acc):
        for c in range(full):
            g = grad[i // slots, i % slots, :, c * LANES : (c + 1) * LANES].astype(jnp.float32)
            acc = acc + g * g
        return acc

    acc = lax.fori_loop(
        0, layers * slots, square, jnp.zeros((rows, LANES), jnp.float32)
    )
    tail = grad[:, :, :, full * LANES :].astype(jnp.float32)
    tail = jnp.sum((tail * tail).reshape(layers * slots * rows, cols - full * LANES), axis=0, keepdims=True)
    acc = jnp.sum(acc, axis=0, keepdims=True)
    part[...] = acc + jnp.concatenate([tail, jnp.zeros_like(tail)], axis=1)
    parts[pl.ds(me, 1)] = part[...].reshape(1, 1, LANES)

    for load in loads[1:]:
        load.wait()

    my_move = [plan[layer, me] % slots for layer in range(layers)]

    def units(x):
        return x.reshape(rows // SUB, SUB, LANES)

    def joined(x):
        x = x.reshape(rows // SUB // 2, 2, SUB, cols - full * LANES)
        return jnp.concatenate([x[:, 0], x[:, 1]], axis=-1)

    for i, ref in enumerate((master, one, two, grad)):
        for c in range(full):
            x = ref[0, my_move[0], :, c * LANES : (c + 1) * LANES].astype(jnp.float32)
            send_raw[4 * c : 4 * c + 4, i] = units(x)
        x = ref[0, my_move[0], :, full * LANES :].astype(jnp.float32)
        send_raw[4 * full : 4 * full + 2, i] = joined(x)

    pl.semaphore_wait(barrier, len(MOVES) + DP - 1)

    part_copies = []
    for k, t in enumerate(targets):
        copy = pltpu.make_async_remote_copy(
            part, parts.at[me], part_send.at[k], part_recv.at[k], device_id={"expert": t}
        )
        copy.start()
        part_copies.append(copy)

    def out(send, hold, layer, start):
        for k, t in enumerate(targets):
            copy = pltpu.make_async_remote_copy(
                send.at[pl.ds(PIECE * t, PIECE)],
                hold.at[me],
                out_send.at[layer, k],
                out_recv.at[layer, k],
                device_id={"expert": t},
            )
            if start:

                @pl.when(t < HOLDERS)
                def _():
                    copy.start()
            else:

                @pl.when(t < HOLDERS)
                def _():
                    copy.wait_send()

    def arrived(send, hold, layer):
        @pl.when(me < HOLDERS)
        def _():
            for k, t in enumerate(targets):
                pltpu.make_async_remote_copy(
                    send.at[pl.ds(0, PIECE)],
                    hold.at[me],
                    out_send.at[layer, k],
                    out_recv.at[layer, k],
                    device_id={"expert": t},
                ).wait_recv()

    def back(buf, layer, start):
        @pl.when(me < HOLDERS)
        def _():
            for k, t in enumerate(targets):
                copy = pltpu.make_async_remote_copy(
                    buf.at[t],
                    home.at[layer, pl.ds(PIECE * me, PIECE)],
                    back_send.at[layer, k],
                    back_recv.at[layer, k],
                    device_id={"expert": t},
                )
                if start:
                    copy.start()
                else:
                    copy.wait_send()

    def returned(buf, layer):
        for k, s in enumerate(sources):

            @pl.when(s < HOLDERS)
            def _():
                pltpu.make_async_remote_copy(
                    buf.at[0],
                    home.at[layer, pl.ds(0, PIECE)],
                    back_send.at[layer, k],
                    back_recv.at[layer, k],
                    device_id={"expert": s},
                ).wait_recv()

    out(send_raw, hold_raw, 0, True)
    hold_raw[pl.ds(me, 1)] = send_raw[pl.ds(PIECE * me, PIECE)][None]

    for copy in part_copies:
        copy.wait_recv()
    plane = jnp.sum(parts[...].reshape(GROUP, LANES), axis=0, keepdims=True)
    line[...] = plane
    lines[pl.ds(dp, 1)] = plane.reshape(1, 1, LANES)
    line_copies = []
    for d in range(1, DP):
        copy = pltpu.make_async_remote_copy(
            line,
            lines.at[dp],
            line_send.at[d - 1],
            line_recv.at[d - 1],
            device_id={"dp": (dp + d) % DP},
        )
        copy.start()
        line_copies.append(copy)
    for copy in line_copies:
        copy.wait_recv()
    total = jnp.sum(lines[...].reshape(DP, LANES), axis=0, keepdims=True)
    total = jnp.sum(total, axis=1, keepdims=True)
    scale = jnp.minimum(1.0, CLIP_RMS * math.sqrt(entry_count) / (jnp.sqrt(total) + 1e-06))

    for c in range(full):
        at = (1, my_move[1], slice(None), slice(c * LANES, (c + 1) * LANES))
        done = adam(master[at], one[at], two[at], grad[at].astype(jnp.float32), scale)
        for i, x in enumerate(done):
            send_new[4 * c : 4 * c + 4, i] = units(x)
    at = (1, my_move[1], slice(None), slice(full * LANES, cols))
    done = adam(master[at], one[at], two[at], grad[at].astype(jnp.float32), scale)
    for i, x in enumerate(done):
        send_new[4 * full : 4 * full + 2, i] = joined(x)
    out(send_new, hold_new, 1, True)
    hold_new[pl.ds(me, 1)] = send_new[pl.ds(PIECE * me, PIECE)][None]

    def resident(i, _):
        layer, slot = i // slots, i % slots
        for lo in range(0, cols, 2 * LANES):
            at = (layer, slot, slice(None), slice(lo, min(lo + 2 * LANES, cols)))
            done = adam(master[at], one[at], two[at], grad[at].astype(jnp.float32), scale)
            for ref, x in zip((new_w, new_one, new_two), done):
                ref[at] = x
        return 0

    lax.fori_loop(0, layers * slots, resident, 0)

    arrived(send_raw, hold_raw, 0)

    def forward_raw(t, _):
        x = hold_raw[plan[0, t] // slots]
        done = adam(x[:, 0], x[:, 1], x[:, 2], x[:, 3], scale)
        for i, y in enumerate(done):
            back_0[t, :, i] = y
        return 0

    lax.fori_loop(0, GROUP, forward_raw, 0)
    back(back_0, 0, True)

    @pl.when(me < HOLDERS)
    def _():
        home[0, pl.ds(PIECE * me, PIECE)] = back_0[me]

    arrived(send_new, hold_new, 1)

    def forward_new(t, _):
        back_1[t] = hold_new[plan[1, t] // slots]
        return 0

    lax.fori_loop(0, GROUP, forward_new, 0)
    back(back_1, 1, True)

    @pl.when(me < HOLDERS)
    def _():
        home[1, pl.ds(PIECE * me, PIECE)] = back_1[me]

    def unpack(layer):
        for i in range(3):
            for c in range(full):
                x = home[layer, 4 * c : 4 * c + 4, i]
                landed[i, layer, :, c * LANES : (c + 1) * LANES] = x.reshape(rows, LANES)
            x = home[layer, 4 * full : 4 * full + 2, i]
            width = cols - full * LANES
            x = jnp.stack([x[:, :, :width], x[:, :, width:]], axis=1)
            landed[i, layer, :, full * LANES :] = x.reshape(rows, width)

    returned(back_0, 0)
    unpack(0)
    returned(back_1, 1)
    unpack(1)

    for copy in part_copies:
        copy.wait_send()
    for copy in line_copies:
        copy.wait_send()
    out(send_raw, hold_raw, 0, False)
    out(send_new, hold_new, 1, False)
    back(back_0, 0, False)
    back(back_1, 1, False)


def exchange(plan, master, moment_one, moment_two, gradient, entry_count):
    layers, slots, rows, cols = master.shape
    vmem = pl.BlockSpec(memory_space=pltpu.VMEM)
    f32 = jnp.float32
    units = PIECE * GROUP
    dma = pltpu.SemaphoreType.DMA
    peers = len(MOVES)
    return pl.pallas_call(
        functools.partial(exchange_kernel, entry_count),
        out_shape=[jax.ShapeDtypeStruct(master.shape, f32)] * 3
        + [jax.ShapeDtypeStruct((3, layers, rows, cols), f32)],
        in_specs=[pl.BlockSpec(memory_space=pltpu.SMEM)] + [pl.BlockSpec(memory_space=pl.ANY)] * 4,
        out_specs=[vmem] * 4,
        scratch_shapes=[
            pltpu.VMEM(master.shape, f32),
            pltpu.VMEM(master.shape, f32),
            pltpu.VMEM(master.shape, f32),
            pltpu.VMEM(master.shape, jnp.bfloat16),
            pltpu.VMEM((units, 4, SUB, LANES), f32),
            pltpu.VMEM((units, 3, SUB, LANES), f32),
            pltpu.VMEM((GROUP, PIECE, 4, SUB, LANES), f32),
            pltpu.VMEM((GROUP, PIECE, 3, SUB, LANES), f32),
            pltpu.VMEM((GROUP, PIECE, 3, SUB, LANES), f32),
            pltpu.VMEM((GROUP, PIECE, 3, SUB, LANES), f32),
            pltpu.VMEM((layers, units, 3, SUB, LANES), f32),
            pltpu.VMEM((1, LANES), f32),
            pltpu.VMEM((GROUP, 1, LANES), f32),
            pltpu.VMEM((1, LANES), f32),
            pltpu.VMEM((DP, 1, LANES), f32),
            dma((4,)),
            dma((peers,)),
            dma((peers,)),
            dma((DP - 1,)),
            dma((DP - 1,)),
            dma((layers, peers)),
            dma((layers, peers)),
            dma((layers, peers)),
            dma((layers, peers)),
        ],
        compiler_params=pltpu.CompilerParams(
            collective_id=0, has_side_effects=True, vmem_limit_bytes=40 * 1024 * 1024
        ),
        name="exchange",
    )(plan, master, moment_one, moment_two, gradient)


def place_kernel(plan, mine, w, one, two, landed, out_w, out_one, out_two, sem):
    layers, slots = w.shape[:2]
    for phase in (0, 1):
        for layer in range(layers):
            moved = plan[layer, mine[0]] % slots
            for i, (src, dst) in enumerate(((w, out_w), (one, out_one), (two, out_two))):
                for slot in range(slots):

                    @pl.when(slot != moved)
                    def _():
                        copy = pltpu.make_async_copy(
                            src.at[layer, slot], dst.at[layer, slot], sem.at[i, layer, slot]
                        )
                        copy.start() if phase == 0 else copy.wait()

                    @pl.when(slot == moved)
                    def _():
                        copy = pltpu.make_async_copy(
                            landed.at[i, layer], dst.at[layer, slot], sem.at[i, layer, slot]
                        )
                        copy.start() if phase == 0 else copy.wait()


def place(plan, mine, w, one, two, landed):
    layers, slots = w.shape[:2]
    vmem = pl.BlockSpec(memory_space=pltpu.VMEM)
    smem = pl.BlockSpec(memory_space=pltpu.SMEM)
    return pl.pallas_call(
        place_kernel,
        out_shape=[jax.ShapeDtypeStruct(w.shape, w.dtype)] * 3,
        in_specs=[smem, smem] + [vmem] * 4,
        out_specs=[pl.BlockSpec(memory_space=pl.ANY)] * 3,
        scratch_shapes=[pltpu.SemaphoreType.DMA((3, layers, slots))],
        name="place",
    )(plan, mine, w, one, two, landed)


def shards(master, moment_one, moment_two, gradient, old_slot, new_slot):
    layers, slots, rows, cols = master.shape
    entry_count = layers * slots * GROUP * rows * DP * cols
    moved = old_slot != new_slot
    word = (old_slot // slots) * slots + new_slot % slots
    here = (new_slot // slots)[:, None, :] == lax.broadcasted_iota(
        jnp.int32, (layers, GROUP, GROUP * slots), 1
    )
    plan = jnp.sum(jnp.where(here & moved[:, None, :], word[:, None, :], 0), axis=2)
    mine = lax.axis_index("expert").reshape(1)
    w, one, two, landed = exchange(plan, master, moment_one, moment_two, gradient, entry_count)
    return place(plan, mine, w, one, two, landed)


def solution(mesh):
    spec = P(None, "expert", "dp", None)
    return jax.shard_map(
        shards,
        mesh=mesh,
        in_specs=(spec, spec, spec, spec, P(), P()),
        out_specs=(spec, spec, spec),
        check_vma=False,
    )
```

```python
import functools
import math

import jax
import jax.numpy as jnp
from jax import lax
from jax.experimental import pallas as pl
from jax.experimental.pallas import tpu as pltpu
from jax.sharding import PartitionSpec as P

BETA_ONE = 0.9
BETA_TWO = 0.95
LEARN_RATE = 0.05
DECAY_RATE = 0.1
ADAM_EPS = 1e-08
CLIP_RMS = 2.0
FIRST_FIX = 1.0 - 0.9**10
SECOND_FIX = 1.0 - 0.95**10

ZDIM, YDIM, CORES = 4, 4, 2
GROUP = ZDIM * YDIM * CORES
DP = 4
LANES = 128
SUB = 4
PIECE = 3
HOLDERS = 30


def move_order():
    moves = [
        (dz, dy, dc)
        for dz in (0, 1, 2, -1)
        for dy in (0, 1, 2, -1)
        for dc in (0, 1)
        if (dz, dy, dc) != (0, 0, 0)
    ]
    neg = lambda v: v if v == 2 else -v
    order = []
    for dz, dy, dc in sorted(moves, key=lambda m: -(abs(m[0]) + abs(m[1]))):
        for m in ((dz, dy, dc), (neg(dz), neg(dy), dc), (dy, dz, dc), (neg(dy), neg(dz), dc)):
            if m not in order:
                order.append(m)
    return order


MOVES = move_order()


def shifted(me, move, sign=1):
    dz, dy, dc = move
    core, y, z = me % CORES, (me // CORES) % YDIM, me // (CORES * YDIM)
    z = (z + sign * dz + ZDIM) % ZDIM
    y = (y + sign * dy + YDIM) % YDIM
    return (z * YDIM + y) * CORES + (core + dc) % CORES


def adam(master, moment_one, moment_two, gradient, scale):
    scaled = gradient * scale
    first = BETA_ONE * moment_one + (1.0 - BETA_ONE) * scaled
    second = BETA_TWO * moment_two + (1.0 - BETA_TWO) * scaled * scaled
    step = (first * (1.0 / FIRST_FIX)) / (jnp.sqrt(second * (1.0 / SECOND_FIX)) + ADAM_EPS)
    return master - LEARN_RATE * (step + DECAY_RATE * master), first, second


def exchange_kernel(
    entry_count,
    master_hbm,
    one_hbm,
    two_hbm,
    grad_hbm,
    old_hbm,
    new_hbm,
    new_w,
    new_one,
    new_two,
    landed,
    plan,
    old,
    new,
    plan_rows,
    master,
    one,
    two,
    grad,
    send_raw,
    send_new,
    hold_raw,
    hold_new,
    back_0,
    back_1,
    home,
    part,
    parts,
    line,
    lines,
    load_sem,
    part_send,
    part_recv,
    line_send,
    line_recv,
    out_send,
    out_recv,
    back_send,
    back_recv,
):
    layers, slots, rows, cols = master.shape
    full = cols // LANES
    dp = lax.axis_index("dp")
    me = lax.axis_index("expert")
    targets = [shifted(me, m) for m in MOVES]
    sources = [shifted(me, m, -1) for m in MOVES]

    loads = [
        pltpu.make_async_copy(src, dst, load_sem.at[i])
        for i, (src, dst) in enumerate(
            (
                (old_hbm, old),
                (new_hbm, new),
                (grad_hbm, grad),
                (master_hbm, master),
                (one_hbm, one),
                (two_hbm, two),
            )
        )
    ]
    for load in loads:
        load.start()

    barrier = pltpu.get_barrier_semaphore()
    for t in targets:
        pl.semaphore_signal(barrier, inc=1, device_id={"expert": t})
    for d in range(1, DP):
        pl.semaphore_signal(barrier, inc=1, device_id={"dp": (dp + d) % DP})

    loads[0].wait()
    loads[1].wait()
    here = lax.broadcasted_iota(jnp.int32, (GROUP, GROUP * slots), 0)
    diagonal = lax.broadcasted_iota(jnp.int32, (GROUP, GROUP), 0) == lax.broadcasted_iota(
        jnp.int32, (GROUP, GROUP), 1
    )
    for layer in range(layers):
        was, now = old[layer : layer + 1], new[layer : layer + 1]
        word = jnp.where(was != now, (was // slots) * slots + now % slots, 0)
        word = jnp.where(now // slots == here, word, 0)
        word = jnp.sum(word, axis=1, keepdims=True)
        plan_rows[layer : layer + 1] = jnp.sum(jnp.where(diagonal, word, 0), axis=0, keepdims=True)
    plan_copy = pltpu.make_async_copy(plan_rows, plan, load_sem.at[6])
    plan_copy.start()

    loads[2].wait()

    def square(i, acc):
        for c in range(full):
            g = grad[i // slots, i % slots, :, c * LANES : (c + 1) * LANES].astype(jnp.float32)
            acc = acc + g * g
        return acc

    acc = lax.fori_loop(
        0, layers * slots, square, jnp.zeros((rows, LANES), jnp.float32)
    )
    tail = grad[:, :, :, full * LANES :].astype(jnp.float32)
    tail = jnp.sum((tail * tail).reshape(layers * slots * rows, cols - full * LANES), axis=0, keepdims=True)
    acc = jnp.sum(acc, axis=0, keepdims=True)
    part[...] = acc + jnp.concatenate([tail, jnp.zeros_like(tail)], axis=1)
    parts[pl.ds(me, 1)] = part[...].reshape(1, 1, LANES)

    for load in loads[3:]:
        load.wait()
    plan_copy.wait()

    my_move = [plan[layer, me] % slots for layer in range(layers)]

    def units(x):
        return x.reshape(rows // SUB, SUB, LANES)

    def joined(x):
        x = x.reshape(rows // SUB // 2, 2, SUB, cols - full * LANES)
        return jnp.concatenate([x[:, 0], x[:, 1]], axis=-1)

    for i, ref in enumerate((master, one, two, grad)):
        for c in range(full):
            x = ref[0, my_move[0], :, c * LANES : (c + 1) * LANES].astype(jnp.float32)
            send_raw[4 * c : 4 * c + 4, i] = units(x)
        x = ref[0, my_move[0], :, full * LANES :].astype(jnp.float32)
        send_raw[4 * full : 4 * full + 2, i] = joined(x)

    pl.semaphore_wait(barrier, len(MOVES) + DP - 1)

    part_copies = []
    for k, t in enumerate(targets):
        copy = pltpu.make_async_remote_copy(
            part, parts.at[me], part_send.at[k], part_recv.at[k], device_id={"expert": t}
        )
        copy.start()
        part_copies.append(copy)

    def out(send, hold, layer, start):
        for k, t in enumerate(targets):
            copy = pltpu.make_async_remote_copy(
                send.at[pl.ds(PIECE * t, PIECE)],
                hold.at[me],
                out_send.at[layer, k],
                out_recv.at[layer, k],
                device_id={"expert": t},
            )
            if start:

                @pl.when(t < HOLDERS)
                def _():
                    copy.start()
            else:

                @pl.when(t < HOLDERS)
                def _():
                    copy.wait_send()

    def arrived(send, hold, layer):
        @pl.when(me < HOLDERS)
        def _():
            for k, t in enumerate(targets):
                pltpu.make_async_remote_copy(
                    send.at[pl.ds(0, PIECE)],
                    hold.at[me],
                    out_send.at[layer, k],
                    out_recv.at[layer, k],
                    device_id={"expert": t},
                ).wait_recv()

    def back(buf, layer, start):
        @pl.when(me < HOLDERS)
        def _():
            for k, t in enumerate(targets):
                copy = pltpu.make_async_remote_copy(
                    buf.at[t],
                    home.at[layer, pl.ds(PIECE * me, PIECE)],
                    back_send.at[layer, k],
                    back_recv.at[layer, k],
                    device_id={"expert": t},
                )
                if start:
                    copy.start()
                else:
                    copy.wait_send()

    def returned(buf, layer):
        for k, s in enumerate(sources):

            @pl.when(s < HOLDERS)
            def _():
                pltpu.make_async_remote_copy(
                    buf.at[0],
                    home.at[layer, pl.ds(0, PIECE)],
                    back_send.at[layer, k],
                    back_recv.at[layer, k],
                    device_id={"expert": s},
                ).wait_recv()

    out(send_raw, hold_raw, 0, True)
    hold_raw[pl.ds(me, 1)] = send_raw[pl.ds(PIECE * me, PIECE)][None]

    for copy in part_copies:
        copy.wait_recv()
    plane = jnp.sum(parts[...].reshape(GROUP, LANES), axis=0, keepdims=True)
    line[...] = plane
    lines[pl.ds(dp, 1)] = plane.reshape(1, 1, LANES)
    line_copies = []
    for d in range(1, DP):
        copy = pltpu.make_async_remote_copy(
            line,
            lines.at[dp],
            line_send.at[d - 1],
            line_recv.at[d - 1],
            device_id={"dp": (dp + d) % DP},
        )
        copy.start()
        line_copies.append(copy)
    for copy in line_copies:
        copy.wait_recv()
    total = jnp.sum(lines[...].reshape(DP, LANES), axis=0, keepdims=True)
    total = jnp.sum(total, axis=1, keepdims=True)
    scale = jnp.minimum(1.0, CLIP_RMS * math.sqrt(entry_count) / (jnp.sqrt(total) + 1e-06))

    for c in range(full):
        at = (1, my_move[1], slice(None), slice(c * LANES, (c + 1) * LANES))
        done = adam(master[at], one[at], two[at], grad[at].astype(jnp.float32), scale)
        for i, x in enumerate(done):
            send_new[4 * c : 4 * c + 4, i] = units(x)
    at = (1, my_move[1], slice(None), slice(full * LANES, cols))
    done = adam(master[at], one[at], two[at], grad[at].astype(jnp.float32), scale)
    for i, x in enumerate(done):
        send_new[4 * full : 4 * full + 2, i] = joined(x)
    out(send_new, hold_new, 1, True)
    hold_new[pl.ds(me, 1)] = send_new[pl.ds(PIECE * me, PIECE)][None]

    def resident(i, _):
        layer, slot = i // slots, i % slots
        for lo in range(0, cols, 2 * LANES):
            at = (layer, slot, slice(None), slice(lo, min(lo + 2 * LANES, cols)))
            done = adam(master[at], one[at], two[at], grad[at].astype(jnp.float32), scale)
            for ref, x in zip((new_w, new_one, new_two), done):
                ref[at] = x
        return 0

    lax.fori_loop(0, layers * slots, resident, 0)

    arrived(send_raw, hold_raw, 0)

    def forward_raw(t, _):
        x = hold_raw[plan[0, t] // slots]
        done = adam(x[:, 0], x[:, 1], x[:, 2], x[:, 3], scale)
        for i, y in enumerate(done):
            back_0[t, :, i] = y
        return 0

    lax.fori_loop(0, GROUP, forward_raw, 0)
    back(back_0, 0, True)

    @pl.when(me < HOLDERS)
    def _():
        home[0, pl.ds(PIECE * me, PIECE)] = back_0[me]

    arrived(send_new, hold_new, 1)

    def forward_new(t, _):
        back_1[t] = hold_new[plan[1, t] // slots]
        return 0

    lax.fori_loop(0, GROUP, forward_new, 0)
    back(back_1, 1, True)

    @pl.when(me < HOLDERS)
    def _():
        home[1, pl.ds(PIECE * me, PIECE)] = back_1[me]

    def unpack(layer):
        for i in range(3):
            for c in range(full):
                x = home[layer, 4 * c : 4 * c + 4, i]
                landed[i, layer, :, c * LANES : (c + 1) * LANES] = x.reshape(rows, LANES)
            x = home[layer, 4 * full : 4 * full + 2, i]
            width = cols - full * LANES
            x = jnp.stack([x[:, :, :width], x[:, :, width:]], axis=1)
            landed[i, layer, :, full * LANES :] = x.reshape(rows, width)

    returned(back_0, 0)
    unpack(0)
    returned(back_1, 1)
    unpack(1)

    for copy in part_copies:
        copy.wait_send()
    for copy in line_copies:
        copy.wait_send()
    out(send_raw, hold_raw, 0, False)
    out(send_new, hold_new, 1, False)
    back(back_0, 0, False)
    back(back_1, 1, False)


def exchange(master, moment_one, moment_two, gradient, old_slot, new_slot, entry_count):
    layers, slots, rows, cols = master.shape
    vmem = pl.BlockSpec(memory_space=pltpu.VMEM)
    f32 = jnp.float32
    units = PIECE * GROUP
    dma = pltpu.SemaphoreType.DMA
    peers = len(MOVES)
    return pl.pallas_call(
        functools.partial(exchange_kernel, entry_count),
        out_shape=[jax.ShapeDtypeStruct(master.shape, f32)] * 3
        + [
            jax.ShapeDtypeStruct((3, layers, rows, cols), f32),
            jax.ShapeDtypeStruct((layers, GROUP), jnp.int32),
        ],
        in_specs=[pl.BlockSpec(memory_space=pltpu.HBM)] * 6,
        out_specs=[vmem] * 4 + [pl.BlockSpec(memory_space=pltpu.SMEM)],
        scratch_shapes=[
            pltpu.VMEM(old_slot.shape, jnp.int32),
            pltpu.VMEM(new_slot.shape, jnp.int32),
            pltpu.VMEM((layers, GROUP), jnp.int32),
            pltpu.VMEM(master.shape, f32),
            pltpu.VMEM(master.shape, f32),
            pltpu.VMEM(master.shape, f32),
            pltpu.VMEM(master.shape, jnp.bfloat16),
            pltpu.VMEM((units, 4, SUB, LANES), f32),
            pltpu.VMEM((units, 3, SUB, LANES), f32),
            pltpu.VMEM((GROUP, PIECE, 4, SUB, LANES), f32),
            pltpu.VMEM((GROUP, PIECE, 3, SUB, LANES), f32),
            pltpu.VMEM((GROUP, PIECE, 3, SUB, LANES), f32),
            pltpu.VMEM((GROUP, PIECE, 3, SUB, LANES), f32),
            pltpu.VMEM((layers, units, 3, SUB, LANES), f32),
            pltpu.VMEM((1, LANES), f32),
            pltpu.VMEM((GROUP, 1, LANES), f32),
            pltpu.VMEM((1, LANES), f32),
            pltpu.VMEM((DP, 1, LANES), f32),
            dma((7,)),
            dma((peers,)),
            dma((peers,)),
            dma((DP - 1,)),
            dma((DP - 1,)),
            dma((layers, peers)),
            dma((layers, peers)),
            dma((layers, peers)),
            dma((layers, peers)),
        ],
        compiler_params=pltpu.CompilerParams(
            collective_id=0, has_side_effects=True, vmem_limit_bytes=40 * 1024 * 1024
        ),
        name="exchange",
    )(
        *(
            pltpu.with_memory_space_constraint(x, pltpu.HBM)
            for x in (master, moment_one, moment_two, gradient, old_slot, new_slot)
        )
    )


def place_kernel(plan, w, one, two, landed, out_w, out_one, out_two, sem):
    layers, slots = w.shape[:2]
    for phase in (0, 1):
        for layer in range(layers):
            moved = plan[layer, lax.axis_index("expert")] % slots
            for i, (src, dst) in enumerate(((w, out_w), (one, out_one), (two, out_two))):
                for slot in range(slots):

                    @pl.when(slot != moved)
                    def _():
                        copy = pltpu.make_async_copy(
                            src.at[layer, slot], dst.at[layer, slot], sem.at[i, layer, slot]
                        )
                        copy.start() if phase == 0 else copy.wait()

                    @pl.when(slot == moved)
                    def _():
                        copy = pltpu.make_async_copy(
                            landed.at[i, layer], dst.at[layer, slot], sem.at[i, layer, slot]
                        )
                        copy.start() if phase == 0 else copy.wait()


def place(plan, w, one, two, landed):
    layers, slots = w.shape[:2]
    return pl.pallas_call(
        place_kernel,
        out_shape=[jax.ShapeDtypeStruct(w.shape, w.dtype)] * 3,
        in_specs=[pl.BlockSpec(memory_space=pltpu.SMEM)] + [pl.BlockSpec(memory_space=pl.ANY)] * 4,
        out_specs=[pl.BlockSpec(memory_space=pl.ANY)] * 3,
        scratch_shapes=[pltpu.SemaphoreType.DMA((3, layers, slots))],
        compiler_params=pltpu.CompilerParams(vmem_limit_bytes=1024 * 1024),
        name="place",
    )(plan, w, one, two, landed)


def shards(master, moment_one, moment_two, gradient, old_slot, new_slot):
    layers, slots, rows, cols = master.shape
    entry_count = layers * slots * GROUP * rows * DP * cols
    w, one, two, landed, plan = exchange(
        master, moment_one, moment_two, gradient, old_slot, new_slot, entry_count
    )
    return place(plan, w, one, two, landed)


def solution(mesh):
    spec = P(None, "expert", "dp", None)
    return jax.shard_map(
        shards,
        mesh=mesh,
        in_specs=(spec, spec, spec, spec, P(), P()),
        out_specs=(spec, spec, spec),
        check_vma=False,
    )
```

```python
import functools
import math

import jax
import jax.numpy as jnp
from jax import lax
from jax.experimental import pallas as pl
from jax.experimental.pallas import tpu as pltpu
from jax.sharding import PartitionSpec as P

BETA_ONE = 0.9
BETA_TWO = 0.95
LEARN_RATE = 0.05
DECAY_RATE = 0.1
ADAM_EPS = 1e-08
CLIP_RMS = 2.0
FIRST_FIX = 1.0 - 0.9**10
SECOND_FIX = 1.0 - 0.95**10

ZDIM, YDIM, CORES = 4, 4, 2
GROUP = ZDIM * YDIM * CORES
DP = 4
LANES = 128
SUB = 4
PIECE = 3
UNITS = 90


def move_order():
    moves = [
        (dz, dy, dc)
        for dz in (0, 1, 2, -1)
        for dy in (0, 1, 2, -1)
        for dc in (0, 1)
        if (dz, dy, dc) != (0, 0, 0)
    ]
    neg = lambda v: v if v == 2 else -v
    order = []
    for dz, dy, dc in sorted(moves, key=lambda m: -(abs(m[0]) + abs(m[1]))):
        for m in ((dz, dy, dc), (neg(dz), neg(dy), dc), (dy, dz, dc), (neg(dy), neg(dz), dc)):
            if m not in order:
                order.append(m)
    return order


MOVES = move_order()


def shifted(me, move):
    dz, dy, dc = move
    core, y, z = me % CORES, (me // CORES) % YDIM, me // (CORES * YDIM)
    z = (z + dz + ZDIM) % ZDIM
    y = (y + dy + YDIM) % YDIM
    return (z * YDIM + y) * CORES + (core + dc) % CORES


def adam(master, moment_one, moment_two, gradient, scale):
    scaled = gradient * scale
    first = BETA_ONE * moment_one + (1.0 - BETA_ONE) * scaled
    second = BETA_TWO * moment_two + (1.0 - BETA_TWO) * scaled * scaled
    step = (first * (1.0 / FIRST_FIX)) / (jnp.sqrt(second * (1.0 / SECOND_FIX)) + ADAM_EPS)
    return master - LEARN_RATE * (step + DECAY_RATE * master), first, second


def is_short(layer, holder):
    return holder % 5 == (4, 2)[layer]


def offset(layer, holder):
    return PIECE * holder - (holder + (0, 2)[layer]) // 5


def unpack(home, block):
    _, rows, cols = block.shape
    full = cols // LANES
    width = cols - full * LANES
    for i in range(block.shape[0]):
        for c in range(full):
            x = home[4 * c : 4 * c + 4, i]
            block[i, :, c * LANES : (c + 1) * LANES] = x.reshape(rows, LANES)
        x = home[4 * full : 4 * full + 2, i]
        x = jnp.stack([x[:, :, :width], x[:, :, width:]], axis=1)
        block[i, :, full * LANES :] = x.reshape(rows, width)


def exchange_kernel(
    entry_count,
    master_hbm,
    one_hbm,
    two_hbm,
    grad_hbm,
    old_hbm,
    new_hbm,
    new_w,
    new_one,
    new_two,
    landed,
    home_1,
    plan,
    old,
    new,
    plan_rows,
    master,
    one,
    two,
    grad,
    send_raw,
    send_new,
    hold_raw,
    hold_new,
    back_0,
    back_1,
    home_0,
    part,
    parts,
    line,
    lines,
    load_sem,
    part_sem,
    out_sem,
    back_sem,
):
    layers, slots, rows, cols = master.shape
    full = cols // LANES
    dp = lax.axis_index("dp")
    me = lax.axis_index("expert")
    targets = [shifted(me, m) for m in MOVES]
    home_of = (home_0, home_1)

    loads = [
        pltpu.make_async_copy(src, dst, load_sem.at[i])
        for i, (src, dst) in enumerate(
            (
                (old_hbm, old),
                (new_hbm, new),
                (grad_hbm, grad),
                (master_hbm, master),
                (one_hbm, one),
                (two_hbm, two),
            )
        )
    ]
    for load in loads:
        load.start()

    barrier = pltpu.get_barrier_semaphore()
    for t in targets:
        pl.semaphore_signal(barrier, inc=1, device_id={"expert": t})
    for d in range(1, DP):
        pl.semaphore_signal(barrier, inc=1, device_id={"dp": (dp + d) % DP})

    loads[0].wait()
    loads[1].wait()
    here = lax.broadcasted_iota(jnp.int32, (GROUP, GROUP * slots), 0)
    diagonal = lax.broadcasted_iota(jnp.int32, (GROUP, GROUP), 0) == lax.broadcasted_iota(
        jnp.int32, (GROUP, GROUP), 1
    )
    for layer in range(layers):
        was, now = old[layer : layer + 1], new[layer : layer + 1]
        word = jnp.where(was != now, (was // slots) * slots + now % slots, 0)
        word = jnp.where(now // slots == here, word, 0)
        word = jnp.sum(word, axis=1, keepdims=True)
        plan_rows[layer : layer + 1] = jnp.sum(jnp.where(diagonal, word, 0), axis=0, keepdims=True)
    plan_copy = pltpu.make_async_copy(plan_rows, plan, load_sem.at[6])
    plan_copy.start()

    loads[2].wait()

    def square(i, acc):
        for c in range(full):
            g = grad[i // slots, i % slots, :, c * LANES : (c + 1) * LANES].astype(jnp.float32)
            acc = acc + g * g
        return acc

    acc = lax.fori_loop(
        0, layers * slots, square, jnp.zeros((rows, LANES), jnp.float32)
    )
    tail = grad[:, :, :, full * LANES :].astype(jnp.float32)
    tail = jnp.sum((tail * tail).reshape(layers * slots * rows, cols - full * LANES), axis=0, keepdims=True)
    acc = jnp.sum(acc, axis=0, keepdims=True)
    part[...] = acc + jnp.concatenate([tail, jnp.zeros_like(tail)], axis=1)
    parts[pl.ds(me, 1)] = part[...].reshape(1, 1, LANES)

    for load in loads[3:]:
        load.wait()
    plan_copy.wait()

    my_move = [plan[layer, me] % slots for layer in range(layers)]

    def units(x):
        return x.reshape(rows // SUB, SUB, LANES)

    def joined(x):
        x = x.reshape(rows // SUB // 2, 2, SUB, cols - full * LANES)
        return jnp.concatenate([x[:, 0], x[:, 1]], axis=-1)

    for i, ref in enumerate((master, one, two, grad)):
        for c in range(full):
            x = ref[0, my_move[0], :, c * LANES : (c + 1) * LANES].astype(jnp.float32)
            send_raw[4 * c : 4 * c + 4, i] = units(x)
        x = ref[0, my_move[0], :, full * LANES :].astype(jnp.float32)
        send_raw[4 * full : 4 * full + 2, i] = joined(x)

    pl.semaphore_wait(barrier, len(MOVES) + DP - 1)

    for t in targets:
        pltpu.make_async_remote_copy(
            part, parts.at[me], part_sem.at[0], part_sem.at[1], device_id={"expert": t}
        ).start()

    def bytes_of(ref, sem):
        return pltpu.make_async_copy(ref, ref, sem)

    def sized(layer, holder, body):
        short = is_short(layer, holder)

        @pl.when(short)
        def _():
            body(PIECE - 1)

        @pl.when(jnp.logical_not(short))
        def _():
            body(PIECE)

    def out(send, hold, layer):
        for t in targets:

            def start(size):
                pltpu.make_async_remote_copy(
                    send.at[pl.ds(offset(layer, t), size)],
                    hold.at[me, pl.ds(0, size)],
                    out_sem.at[layer, 0],
                    out_sem.at[layer, 1],
                    device_id={"expert": t},
                ).start()

            sized(layer, t, start)

        def keep(size):
            hold[pl.ds(me, 1), 0:size] = send[pl.ds(offset(layer, me), size)][None]

        sized(layer, me, keep)

    def arrived(hold, layer):
        def wait(size):
            bytes_of(hold.at[0 : GROUP - 1, 0:size], out_sem.at[layer, 1]).wait()

        sized(layer, me, wait)

    def back(buf, layer):
        def start(size):
            for t in targets:
                pltpu.make_async_remote_copy(
                    buf.at[t, pl.ds(0, size)],
                    home_of[layer].at[pl.ds(offset(layer, me), size)],
                    back_sem.at[layer, 0],
                    back_sem.at[layer, 1],
                    device_id={"expert": t},
                ).start()
            home_of[layer][pl.ds(offset(layer, me), size)] = buf[me, 0:size]

        sized(layer, me, start)

    def returned(layer):
        def wait(size):
            bytes_of(home_of[layer].at[0 : UNITS - size], back_sem.at[layer, 1]).wait()

        sized(layer, me, wait)

    def sent(send, buf, layer):
        def wait(size):
            bytes_of(send.at[0 : UNITS - size], out_sem.at[layer, 0]).wait()
            bytes_of(buf.at[0 : GROUP - 1, 0:size], back_sem.at[layer, 0]).wait()

        sized(layer, me, wait)

    out(send_raw, hold_raw, 0)

    bytes_of(parts.at[0 : GROUP - 1], part_sem.at[1]).wait()
    plane = jnp.sum(parts[...].reshape(GROUP, LANES), axis=0, keepdims=True)
    line[...] = plane
    lines[pl.ds(dp, 1)] = plane.reshape(1, 1, LANES)
    for d in range(1, DP):
        pltpu.make_async_remote_copy(
            line, lines.at[dp], part_sem.at[2], part_sem.at[3], device_id={"dp": (dp + d) % DP}
        ).start()
    bytes_of(lines.at[0 : DP - 1], part_sem.at[3]).wait()
    total = jnp.sum(lines[...].reshape(DP, LANES), axis=0, keepdims=True)
    total = jnp.sum(total, axis=1, keepdims=True)
    scale = jnp.minimum(1.0, CLIP_RMS * math.sqrt(entry_count) / (jnp.sqrt(total) + 1e-06))

    for c in range(full):
        at = (1, my_move[1], slice(None), slice(c * LANES, (c + 1) * LANES))
        done = adam(master[at], one[at], two[at], grad[at].astype(jnp.float32), scale)
        for i, x in enumerate(done):
            send_new[4 * c : 4 * c + 4, i] = units(x)
    at = (1, my_move[1], slice(None), slice(full * LANES, cols))
    done = adam(master[at], one[at], two[at], grad[at].astype(jnp.float32), scale)
    for i, x in enumerate(done):
        send_new[4 * full : 4 * full + 2, i] = joined(x)
    out(send_new, hold_new, 1)

    def resident(i, _):
        layer, slot = i // slots, i % slots
        for lo in range(0, cols, 2 * LANES):
            at = (layer, slot, slice(None), slice(lo, min(lo + 2 * LANES, cols)))
            done = adam(master[at], one[at], two[at], grad[at].astype(jnp.float32), scale)
            for ref, x in zip((new_w, new_one, new_two), done):
                ref[at] = x
        return 0

    lax.fori_loop(0, layers * slots, resident, 0)

    arrived(hold_raw, 0)

    def forward_raw(t, _):
        x = hold_raw[plan[0, t] // slots]
        done = adam(x[:, 0], x[:, 1], x[:, 2], x[:, 3], scale)
        for i, y in enumerate(done):
            back_0[t, :, i] = y
        return 0

    lax.fori_loop(0, GROUP, forward_raw, 0)
    back(back_0, 0)

    arrived(hold_new, 1)

    def forward_new(t, _):
        back_1[t] = hold_new[plan[1, t] // slots]
        return 0

    lax.fori_loop(0, GROUP, forward_new, 0)
    back(back_1, 1)

    returned(0)
    unpack(home_0, landed)
    returned(1)

    bytes_of(parts.at[0 : GROUP - 1], part_sem.at[0]).wait()
    bytes_of(lines.at[0 : DP - 1], part_sem.at[2]).wait()
    sent(send_raw, back_0, 0)
    sent(send_new, back_1, 1)


def exchange(master, moment_one, moment_two, gradient, old_slot, new_slot, entry_count):
    layers, slots, rows, cols = master.shape
    vmem = pl.BlockSpec(memory_space=pltpu.VMEM)
    f32 = jnp.float32
    dma = pltpu.SemaphoreType.DMA
    return pl.pallas_call(
        functools.partial(exchange_kernel, entry_count),
        out_shape=[jax.ShapeDtypeStruct(master.shape, f32)] * 3
        + [
            jax.ShapeDtypeStruct((3, rows, cols), f32),
            jax.ShapeDtypeStruct((UNITS, 3, SUB, LANES), f32),
            jax.ShapeDtypeStruct((layers, GROUP), jnp.int32),
        ],
        in_specs=[pl.BlockSpec(memory_space=pltpu.HBM)] * 6,
        out_specs=[vmem] * 5 + [pl.BlockSpec(memory_space=pltpu.SMEM)],
        scratch_shapes=[
            pltpu.VMEM(old_slot.shape, jnp.int32),
            pltpu.VMEM(new_slot.shape, jnp.int32),
            pltpu.VMEM((layers, GROUP), jnp.int32),
            pltpu.VMEM(master.shape, f32),
            pltpu.VMEM(master.shape, f32),
            pltpu.VMEM(master.shape, f32),
            pltpu.VMEM(master.shape, jnp.bfloat16),
            pltpu.VMEM((UNITS, 4, SUB, LANES), f32),
            pltpu.VMEM((UNITS, 3, SUB, LANES), f32),
            pltpu.VMEM((GROUP, PIECE, 4, SUB, LANES), f32),
            pltpu.VMEM((GROUP, PIECE, 3, SUB, LANES), f32),
            pltpu.VMEM((GROUP, PIECE, 3, SUB, LANES), f32),
            pltpu.VMEM((GROUP, PIECE, 3, SUB, LANES), f32),
            pltpu.VMEM((UNITS, 3, SUB, LANES), f32),
            pltpu.VMEM((1, LANES), f32),
            pltpu.VMEM((GROUP, 1, LANES), f32),
            pltpu.VMEM((1, LANES), f32),
            pltpu.VMEM((DP, 1, LANES), f32),
            dma((7,)),
            dma((4,)),
            dma((layers, 2)),
            dma((layers, 2)),
        ],
        compiler_params=pltpu.CompilerParams(
            collective_id=0, has_side_effects=True, vmem_limit_bytes=40 * 1024 * 1024
        ),
        name="exchange",
    )(
        *(
            pltpu.with_memory_space_constraint(x, pltpu.HBM)
            for x in (master, moment_one, moment_two, gradient, old_slot, new_slot)
        )
    )


def place_kernel(plan, w, one, two, landed, home, out_w, out_one, out_two, last, sem):
    layers, slots = w.shape[:2]
    pairs = ((w, out_w), (one, out_one), (two, out_two))
    moved = [plan[layer, lax.axis_index("expert")] % slots for layer in range(layers)]
    for layer in range(layers):
        for i, (src, dst) in enumerate(pairs):
            for slot in range(slots):

                @pl.when(slot != moved[layer])
                def _():
                    pltpu.make_async_copy(
                        src.at[layer, slot], dst.at[layer, slot], sem.at[i]
                    ).start()

    unpack(home, last)
    for layer, block in enumerate((landed, last)):
        for i, (_, dst) in enumerate(pairs):
            pltpu.make_async_copy(block.at[i], dst.at[layer, moved[layer]], sem.at[i]).start()
    for i, (src, dst) in enumerate(pairs):
        pltpu.make_async_copy(src, dst, sem.at[i]).wait()


def place(plan, w, one, two, landed, home):
    rows, cols = w.shape[2:]
    vmem = pl.BlockSpec(memory_space=pltpu.VMEM)
    free = pl.BlockSpec(memory_space=pl.ANY)
    return pl.pallas_call(
        place_kernel,
        out_shape=[jax.ShapeDtypeStruct(w.shape, w.dtype)] * 3,
        in_specs=[pl.BlockSpec(memory_space=pltpu.SMEM)] + [free] * 4 + [vmem],
        out_specs=[free] * 3,
        scratch_shapes=[pltpu.VMEM((3, rows, cols), w.dtype), pltpu.SemaphoreType.DMA((3,))],
        compiler_params=pltpu.CompilerParams(vmem_limit_bytes=4 * 1024 * 1024),
        name="place",
    )(plan, w, one, two, landed, home)


def shards(master, moment_one, moment_two, gradient, old_slot, new_slot):
    layers, slots, rows, cols = master.shape
    entry_count = layers * slots * GROUP * rows * DP * cols
    w, one, two, landed, home, plan = exchange(
        master, moment_one, moment_two, gradient, old_slot, new_slot, entry_count
    )
    return place(plan, w, one, two, landed, home)


def solution(mesh):
    spec = P(None, "expert", "dp", None)
    return jax.shard_map(
        shards,
        mesh=mesh,
        in_specs=(spec, spec, spec, spec, P(), P()),
        out_specs=(spec, spec, spec),
        check_vma=False,
    )
```

```python
import functools
import math

import jax
import jax.numpy as jnp
from jax import lax
from jax.experimental import pallas as pl
from jax.experimental.pallas import tpu as pltpu
from jax.sharding import PartitionSpec as P

BETA_ONE = 0.9
BETA_TWO = 0.95
LEARN_RATE = 0.05
DECAY_RATE = 0.1
ADAM_EPS = 1e-08
CLIP_RMS = 2.0
FIRST_FIX = 1.0 - 0.9**10
SECOND_FIX = 1.0 - 0.95**10

ZDIM, YDIM, CORES = 4, 4, 2
GROUP = ZDIM * YDIM * CORES
DP = 4
LANES = 128
SUB = 4
PIECE = 3
UNITS = 90
CHAINS = 6


def move_order():
    moves = [
        (dz, dy, dc)
        for dz in (0, 1, 2, -1)
        for dy in (0, 1, 2, -1)
        for dc in (0, 1)
        if (dz, dy, dc) != (0, 0, 0)
    ]
    neg = lambda v: v if v == 2 else -v
    order = []
    for dz, dy, dc in sorted(moves, key=lambda m: -(abs(m[0]) + abs(m[1]))):
        for m in ((dz, dy, dc), (neg(dz), neg(dy), dc), (dy, dz, dc), (neg(dy), neg(dz), dc)):
            if m not in order:
                order.append(m)
    return order


MOVES = move_order()


def shifted(me, move):
    dz, dy, dc = move
    core, y, z = me % CORES, (me // CORES) % YDIM, me // (CORES * YDIM)
    z = (z + dz + ZDIM) % ZDIM
    y = (y + dy + YDIM) % YDIM
    return (z * YDIM + y) * CORES + (core + dc) % CORES


def adam(master, moment_one, moment_two, gradient, scale):
    scaled = gradient * scale
    first = BETA_ONE * moment_one + (1.0 - BETA_ONE) * scaled
    second = BETA_TWO * moment_two + (1.0 - BETA_TWO) * scaled * scaled
    step = (first * (1.0 / FIRST_FIX)) / (jnp.sqrt(second * (1.0 / SECOND_FIX)) + ADAM_EPS)
    return master - LEARN_RATE * (step + DECAY_RATE * master), first, second


def is_short(layer, holder):
    return holder % 5 == (4, 2)[layer]


def offset(layer, holder):
    return PIECE * holder - (holder + (0, 2)[layer]) // 5


def unpack(home, block):
    _, rows, cols = block.shape
    full = cols // LANES
    width = cols - full * LANES
    for i in range(block.shape[0]):
        for c in range(full):
            x = home[4 * c : 4 * c + 4, i]
            block[i, :, c * LANES : (c + 1) * LANES] = x.reshape(rows, LANES)
        x = home[4 * full : 4 * full + 2, i]
        x = jnp.stack([x[:, :, :width], x[:, :, width:]], axis=1)
        block[i, :, full * LANES :] = x.reshape(rows, width)


def exchange_kernel(
    entry_count,
    master_hbm,
    one_hbm,
    two_hbm,
    grad_hbm,
    old_hbm,
    new_hbm,
    new_w,
    new_one,
    new_two,
    landed,
    home_1,
    plan_rows,
    old,
    new,
    plan,
    master_0,
    master_1,
    one_0,
    one_1,
    two_0,
    two_1,
    grad,
    send_raw,
    send_new,
    hold_raw,
    hold_new,
    back_0,
    back_1,
    home_0,
    part,
    parts,
    line,
    lines,
    load_sem,
    part_sem,
    out_sem,
    back_sem,
):
    layers, slots, rows, cols = master_hbm.shape
    master, one, two = (master_0, master_1), (one_0, one_1), (two_0, two_1)
    full = cols // LANES
    dp = lax.axis_index("dp")
    me = lax.axis_index("expert")
    targets = [shifted(me, m) for m in MOVES]
    orders = (targets[-9:-1] + targets[:-9] + targets[-1:], targets)
    home_of = (home_0, home_1)

    barrier = pltpu.get_barrier_semaphore()
    for t in targets:
        pl.semaphore_signal(barrier, inc=1, device_id={"expert": t})
    for d in range(1, DP):
        pl.semaphore_signal(barrier, inc=1, device_id={"dp": (dp + d) % DP})

    def load(src, dst, sem):
        copy = pltpu.make_async_copy(src, dst, load_sem.at[sem])
        copy.start()
        return copy

    old_load, new_load = load(old_hbm, old, 0), load(new_hbm, new, 1)
    grad_load = load(grad_hbm, grad, 2)
    arrays = ((master_hbm, master), (one_hbm, one), (two_hbm, two))
    loads = [
        [load(src.at[layer], dst[layer], 3 + 3 * layer + i) for i, (src, dst) in enumerate(arrays)]
        for layer in range(layers)
    ]

    old_load.wait()
    new_load.wait()
    here = lax.broadcasted_iota(jnp.int32, (GROUP, GROUP * slots), 0)
    diagonal = lax.broadcasted_iota(jnp.int32, (GROUP, GROUP), 0) == lax.broadcasted_iota(
        jnp.int32, (GROUP, GROUP), 1
    )
    for layer in range(layers):
        was, now = old[layer : layer + 1], new[layer : layer + 1]
        word = jnp.where(was != now, (was // slots) * slots + now % slots, 0)
        word = jnp.where(now // slots == here, word, 0)
        word = jnp.sum(word, axis=1, keepdims=True)
        plan_rows[layer : layer + 1] = jnp.sum(jnp.where(diagonal, word, 0), axis=0, keepdims=True)
    plan_copy = pltpu.make_async_copy(plan_rows, plan, load_sem.at[9])
    plan_copy.start()

    grad_load.wait()

    def square(i, accs):
        accs = list(accs)
        for c in range(full):
            g = grad[i // slots, i % slots, :, c * LANES : (c + 1) * LANES].astype(jnp.float32)
            accs[c % CHAINS] += g * g
        return tuple(accs)

    zero = jnp.zeros((rows, LANES), jnp.float32)
    acc = sum(lax.fori_loop(0, layers * slots, square, (zero,) * CHAINS))
    tail = grad[:, :, :, full * LANES :].astype(jnp.float32)
    tail = jnp.sum((tail * tail).reshape(layers * slots * rows, cols - full * LANES), axis=0, keepdims=True)
    acc = jnp.sum(acc, axis=0, keepdims=True)
    part[...] = acc + jnp.concatenate([tail, jnp.zeros_like(tail)], axis=1)
    parts[pl.ds(me, 1)] = part[...].reshape(1, 1, LANES)

    pl.semaphore_wait(barrier, len(MOVES) + DP - 1)

    for t in targets:
        pltpu.make_async_remote_copy(
            part, parts.at[me], part_sem.at[0], part_sem.at[1], device_id={"expert": t}
        ).start()

    for copy in loads[0]:
        copy.wait()
    plan_copy.wait()

    my_move = [plan[layer, me] % slots for layer in range(layers)]

    def units(x):
        return x.reshape(rows // SUB, SUB, LANES)

    def joined(x):
        x = x.reshape(rows // SUB // 2, 2, SUB, cols - full * LANES)
        return jnp.concatenate([x[:, 0], x[:, 1]], axis=-1)

    for i, ref in enumerate((master_0, one_0, two_0, grad.at[0])):
        for c in range(full):
            x = ref[my_move[0], :, c * LANES : (c + 1) * LANES].astype(jnp.float32)
            send_raw[4 * c : 4 * c + 4, i] = units(x)
        x = ref[my_move[0], :, full * LANES :].astype(jnp.float32)
        send_raw[4 * full : 4 * full + 2, i] = joined(x)

    def bytes_of(ref, sem):
        return pltpu.make_async_copy(ref, ref, sem)

    def sized(layer, holder, body):
        short = is_short(layer, holder)

        @pl.when(short)
        def _():
            body(PIECE - 1)

        @pl.when(jnp.logical_not(short))
        def _():
            body(PIECE)

    def out(send, hold, layer):
        for t in orders[layer]:

            def start(size):
                pltpu.make_async_remote_copy(
                    send.at[pl.ds(offset(layer, t), size)],
                    hold.at[me, pl.ds(0, size)],
                    out_sem.at[layer, 0],
                    out_sem.at[layer, 1],
                    device_id={"expert": t},
                ).start()

            sized(layer, t, start)

    def keep(send, hold, layer):
        def body(size):
            hold[pl.ds(me, 1), 0:size] = send[pl.ds(offset(layer, me), size)][None]

        sized(layer, me, body)

    def arrived(hold, layer):
        def wait(size):
            bytes_of(hold.at[0 : GROUP - 1, 0:size], out_sem.at[layer, 1]).wait()

        sized(layer, me, wait)

    def back(buf, layer):
        def start(size):
            for t in targets:
                pltpu.make_async_remote_copy(
                    buf.at[t, pl.ds(0, size)],
                    home_of[layer].at[pl.ds(offset(layer, me), size)],
                    back_sem.at[layer, 0],
                    back_sem.at[layer, 1],
                    device_id={"expert": t},
                ).start()
            home_of[layer][pl.ds(offset(layer, me), size)] = buf[me, 0:size]

        sized(layer, me, start)

    def returned(layer):
        def wait(size):
            bytes_of(home_of[layer].at[0 : UNITS - size], back_sem.at[layer, 1]).wait()

        sized(layer, me, wait)

    def sent(send, buf, layer):
        def wait(size):
            bytes_of(send.at[0 : UNITS - size], out_sem.at[layer, 0]).wait()
            bytes_of(buf.at[0 : GROUP - 1, 0:size], back_sem.at[layer, 0]).wait()

        sized(layer, me, wait)

    out(send_raw, hold_raw, 0)
    for copy in loads[1]:
        copy.wait()

    bytes_of(parts.at[0 : GROUP - 1], part_sem.at[1]).wait()
    line[...] = jnp.sum(parts[...].reshape(GROUP, LANES), axis=0, keepdims=True)
    lines[pl.ds(dp, 1)] = line[...].reshape(1, 1, LANES)
    for d in range(1, DP):
        pltpu.make_async_remote_copy(
            line, lines.at[dp], part_sem.at[2], part_sem.at[3], device_id={"dp": (dp + d) % DP}
        ).start()
    keep(send_raw, hold_raw, 0)
    bytes_of(lines.at[0 : DP - 1], part_sem.at[3]).wait()
    total = jnp.sum(lines[...].reshape(DP, LANES), axis=0, keepdims=True)
    total = jnp.sum(total, axis=1, keepdims=True)
    scale = jnp.minimum(1.0, CLIP_RMS * math.sqrt(entry_count) / (jnp.sqrt(total) + 1e-06))

    def updated(layer, at):
        return adam(
            master[layer][at],
            one[layer][at],
            two[layer][at],
            grad[(layer, *at)].astype(jnp.float32),
            scale,
        )

    for c in range(full):
        done = updated(1, (my_move[1], slice(None), slice(c * LANES, (c + 1) * LANES)))
        for i, x in enumerate(done):
            send_new[4 * c : 4 * c + 4, i] = units(x)
    done = updated(1, (my_move[1], slice(None), slice(full * LANES, cols)))
    for i, x in enumerate(done):
        send_new[4 * full : 4 * full + 2, i] = joined(x)
    out(send_new, hold_new, 1)
    keep(send_new, hold_new, 1)

    arrived(hold_raw, 0)

    def forward_raw(t, _):
        x = hold_raw[plan[0, t] // slots]
        done = adam(x[:, 0], x[:, 1], x[:, 2], x[:, 3], scale)
        for i, y in enumerate(done):
            back_0[t, :, i] = y
        return 0

    lax.fori_loop(0, GROUP, forward_raw, 0)
    back(back_0, 0)

    for layer in range(layers):

        def resident(slot, _):
            for lo in range(0, cols, 2 * LANES):
                at = (slot, slice(None), slice(lo, min(lo + 2 * LANES, cols)))
                for ref, x in zip((new_w, new_one, new_two), updated(layer, at)):
                    ref[(layer, *at)] = x
            return 0

        lax.fori_loop(0, slots, resident, 0)

    arrived(hold_new, 1)

    def forward_new(t, _):
        back_1[t] = hold_new[plan[1, t] // slots]
        return 0

    lax.fori_loop(0, GROUP, forward_new, 0)
    back(back_1, 1)

    returned(0)
    unpack(home_0, landed)
    returned(1)

    bytes_of(parts.at[0 : GROUP - 1], part_sem.at[0]).wait()
    bytes_of(lines.at[0 : DP - 1], part_sem.at[2]).wait()
    sent(send_raw, back_0, 0)
    sent(send_new, back_1, 1)


def exchange(master, moment_one, moment_two, gradient, old_slot, new_slot, entry_count):
    layers, slots, rows, cols = master.shape
    vmem = pl.BlockSpec(memory_space=pltpu.VMEM)
    f32 = jnp.float32
    dma = pltpu.SemaphoreType.DMA
    return pl.pallas_call(
        functools.partial(exchange_kernel, entry_count),
        out_shape=[jax.ShapeDtypeStruct(master.shape, f32)] * 3
        + [
            jax.ShapeDtypeStruct((3, rows, cols), f32),
            jax.ShapeDtypeStruct((UNITS, 3, SUB, LANES), f32),
            jax.ShapeDtypeStruct((layers, GROUP), jnp.int32),
        ],
        in_specs=[pl.BlockSpec(memory_space=pltpu.HBM)] * 6,
        out_specs=[vmem] * 6,
        scratch_shapes=[
            pltpu.VMEM(old_slot.shape, jnp.int32),
            pltpu.VMEM(new_slot.shape, jnp.int32),
            pltpu.SMEM((layers, GROUP), jnp.int32),
            *[pltpu.VMEM(master.shape[1:], f32)] * (3 * layers),
            pltpu.VMEM(master.shape, jnp.bfloat16),
            pltpu.VMEM((UNITS, 4, SUB, LANES), f32),
            pltpu.VMEM((UNITS, 3, SUB, LANES), f32),
            pltpu.VMEM((GROUP, PIECE, 4, SUB, LANES), f32),
            pltpu.VMEM((GROUP, PIECE, 3, SUB, LANES), f32),
            pltpu.VMEM((GROUP, PIECE, 3, SUB, LANES), f32),
            pltpu.VMEM((GROUP, PIECE, 3, SUB, LANES), f32),
            pltpu.VMEM((UNITS, 3, SUB, LANES), f32),
            pltpu.VMEM((1, LANES), f32),
            pltpu.VMEM((GROUP, 1, LANES), f32),
            pltpu.VMEM((1, LANES), f32),
            pltpu.VMEM((DP, 1, LANES), f32),
            dma((10,)),
            dma((4,)),
            dma((layers, 2)),
            dma((layers, 2)),
        ],
        compiler_params=pltpu.CompilerParams(
            collective_id=0, has_side_effects=True, vmem_limit_bytes=40 * 1024 * 1024
        ),
        name="exchange",
    )(
        *(
            pltpu.with_memory_space_constraint(x, pltpu.HBM)
            for x in (master, moment_one, moment_two, gradient, old_slot, new_slot)
        )
    )


def place_kernel(plan, w, one, two, landed, home, out_w, out_one, out_two, last, sem):
    layers, slots = w.shape[:2]
    pairs = ((w, out_w), (one, out_one), (two, out_two))
    mine = lax.broadcasted_iota(jnp.int32, plan.shape, 1) == lax.axis_index("expert")
    chosen = jnp.where(mine, plan[...], 0)
    moved = [jnp.sum(chosen[layer : layer + 1]) % slots for layer in range(layers)]
    for layer in range(layers):
        for i, (src, dst) in enumerate(pairs):
            for slot in range(slots):

                @pl.when(slot != moved[layer])
                def _():
                    pltpu.make_async_copy(
                        src.at[layer, slot], dst.at[layer, slot], sem.at[i]
                    ).start()

    unpack(home, last)
    for layer, block in enumerate((landed, last)):
        for i, (_, dst) in enumerate(pairs):
            pltpu.make_async_copy(block.at[i], dst.at[layer, moved[layer]], sem.at[i]).start()
    for i, (src, dst) in enumerate(pairs):
        pltpu.make_async_copy(src, dst, sem.at[i]).wait()


def place(plan, w, one, two, landed, home):
    rows, cols = w.shape[2:]
    vmem = pl.BlockSpec(memory_space=pltpu.VMEM)
    free = pl.BlockSpec(memory_space=pl.ANY)
    return pl.pallas_call(
        place_kernel,
        out_shape=[jax.ShapeDtypeStruct(w.shape, w.dtype)] * 3,
        in_specs=[vmem] + [free] * 4 + [vmem],
        out_specs=[free] * 3,
        scratch_shapes=[pltpu.VMEM((3, rows, cols), w.dtype), pltpu.SemaphoreType.DMA((3,))],
        compiler_params=pltpu.CompilerParams(vmem_limit_bytes=4 * 1024 * 1024),
        name="place",
    )(plan, w, one, two, landed, home)


def shards(master, moment_one, moment_two, gradient, old_slot, new_slot):
    layers, slots, rows, cols = master.shape
    entry_count = layers * slots * GROUP * rows * DP * cols
    w, one, two, landed, home, plan = exchange(
        master, moment_one, moment_two, gradient, old_slot, new_slot, entry_count
    )
    return place(plan, w, one, two, landed, home)


def solution(mesh):
    spec = P(None, "expert", "dp", None)
    return jax.shard_map(
        shards,
        mesh=mesh,
        in_specs=(spec, spec, spec, spec, P(), P()),
        out_specs=(spec, spec, spec),
        check_vma=False,
    )
```

```python
import functools
import math

import jax
import jax.numpy as jnp
from jax import lax
from jax.experimental import pallas as pl
from jax.experimental.pallas import tpu as pltpu
from jax.sharding import PartitionSpec as P

BETA_ONE = 0.9
BETA_TWO = 0.95
LEARN_RATE = 0.05
DECAY_RATE = 0.1
ADAM_EPS = 1e-08
CLIP_RMS = 2.0
FIRST_FIX = 1.0 - 0.9**10
SECOND_FIX = 1.0 - 0.95**10

ZDIM, YDIM, CORES = 4, 4, 2
GROUP = ZDIM * YDIM * CORES
DP = 4
LANES = 128
SUB = 4
PIECE = 3
RAW = 2
UNITS = 90
CHAINS = 6


def move_order():
    moves = [
        (dz, dy, dc)
        for dz in (0, 1, 2, -1)
        for dy in (0, 1, 2, -1)
        for dc in (0, 1)
        if (dz, dy, dc) != (0, 0, 0)
    ]
    neg = lambda v: v if v == 2 else -v
    order = []
    for dz, dy, dc in sorted(moves, key=lambda m: -(abs(m[0]) + abs(m[1]))):
        for m in ((dz, dy, dc), (neg(dz), neg(dy), dc), (dy, dz, dc), (neg(dy), neg(dz), dc)):
            if m not in order:
                order.append(m)
    return order


MOVES = move_order()


def shifted(me, move):
    dz, dy, dc = move
    core, y, z = me % CORES, (me // CORES) % YDIM, me // (CORES * YDIM)
    z = (z + dz + ZDIM) % ZDIM
    y = (y + dy + YDIM) % YDIM
    return (z * YDIM + y) * CORES + (core + dc) % CORES


def moments(moment_one, moment_two, gradient, scale):
    scaled = gradient * scale
    first = BETA_ONE * moment_one + (1.0 - BETA_ONE) * scaled
    second = BETA_TWO * moment_two + (1.0 - BETA_TWO) * scaled * scaled
    return first, second


def stepped(master, first, second):
    step = (first * (1.0 / FIRST_FIX)) / (jnp.sqrt(second * (1.0 / SECOND_FIX)) + ADAM_EPS)
    return master - LEARN_RATE * (step + DECAY_RATE * master)


def adam(master, moment_one, moment_two, gradient, scale):
    first, second = moments(moment_one, moment_two, gradient, scale)
    return stepped(master, first, second), first, second


def is_short(layer, holder):
    return holder % 5 == (4, 2)[layer]


def offset(layer, holder):
    return PIECE * holder - (holder + (0, 2)[layer]) // 5


def unpack(home, block):
    _, rows, cols = block.shape
    full = cols // LANES
    width = cols - full * LANES
    for i in range(block.shape[0]):
        for c in range(full):
            x = home[4 * c : 4 * c + 4, i]
            block[i, :, c * LANES : (c + 1) * LANES] = x.reshape(rows, LANES)
        x = home[4 * full : 4 * full + 2, i]
        x = jnp.stack([x[:, :, :width], x[:, :, width:]], axis=1)
        block[i, :, full * LANES :] = x.reshape(rows, width)


def exchange_kernel(
    entry_count,
    master_hbm,
    one_hbm,
    two_hbm,
    grad_hbm,
    old_hbm,
    new_hbm,
    new_w,
    new_one,
    new_two,
    landed,
    home_1,
    plan_rows,
    old,
    new,
    plan,
    master_0,
    master_1,
    one_0,
    one_1,
    two_0,
    two_1,
    grad,
    send_raw,
    send_master,
    send_rest,
    send_new,
    hold_raw,
    hold_master,
    hold_rest,
    hold_new,
    back_0,
    back_rest,
    back_1,
    home_0,
    part,
    parts,
    line,
    lines,
    load_sem,
    part_sem,
    out_sem,
    back_sem,
):
    layers, slots, rows, cols = master_hbm.shape
    master, one, two = (master_0, master_1), (one_0, one_1), (two_0, two_1)
    full = cols // LANES
    dp = lax.axis_index("dp")
    me = lax.axis_index("expert")
    targets = [shifted(me, m) for m in MOVES]
    near_first = targets[-9:-1] + targets[:-9] + targets[-1:]

    barrier = pltpu.get_barrier_semaphore()
    for t in targets:
        pl.semaphore_signal(barrier, inc=1, device_id={"expert": t})
    for d in range(1, DP):
        pl.semaphore_signal(barrier, inc=1, device_id={"dp": (dp + d) % DP})

    def load(src, dst, sem):
        copy = pltpu.make_async_copy(src, dst, load_sem.at[sem])
        copy.start()
        return copy

    old_load, new_load = load(old_hbm, old, 0), load(new_hbm, new, 1)
    grad_load = load(grad_hbm, grad, 2)
    arrays = ((master_hbm, master), (one_hbm, one), (two_hbm, two))
    loads = [
        [load(src.at[layer], dst[layer], 3 + 3 * layer + i) for i, (src, dst) in enumerate(arrays)]
        for layer in range(layers)
    ]

    old_load.wait()
    new_load.wait()
    here = lax.broadcasted_iota(jnp.int32, (GROUP, GROUP * slots), 0)
    diagonal = lax.broadcasted_iota(jnp.int32, (GROUP, GROUP), 0) == lax.broadcasted_iota(
        jnp.int32, (GROUP, GROUP), 1
    )
    for layer in range(layers):
        was, now = old[layer : layer + 1], new[layer : layer + 1]
        word = jnp.where(was != now, (was // slots) * slots + now % slots, 0)
        word = jnp.where(now // slots == here, word, 0)
        word = jnp.sum(word, axis=1, keepdims=True)
        plan_rows[layer : layer + 1] = jnp.sum(jnp.where(diagonal, word, 0), axis=0, keepdims=True)
    plan_copy = pltpu.make_async_copy(plan_rows, plan, load_sem.at[9])
    plan_copy.start()

    grad_load.wait()

    def square(i, accs):
        accs = list(accs)
        for c in range(full):
            g = grad[i // slots, i % slots, :, c * LANES : (c + 1) * LANES].astype(jnp.float32)
            accs[c % CHAINS] += g * g
        return tuple(accs)

    zero = jnp.zeros((rows, LANES), jnp.float32)
    acc = sum(lax.fori_loop(0, layers * slots, square, (zero,) * CHAINS))
    tail = grad[:, :, :, full * LANES :].astype(jnp.float32)
    tail = jnp.sum((tail * tail).reshape(layers * slots * rows, cols - full * LANES), axis=0, keepdims=True)
    acc = jnp.sum(acc, axis=0, keepdims=True)
    part[...] = acc + jnp.concatenate([tail, jnp.zeros_like(tail)], axis=1)
    parts[pl.ds(me, 1)] = part[...].reshape(1, 1, LANES)

    pl.semaphore_wait(barrier, len(MOVES) + DP - 1)

    for t in targets:
        pltpu.make_async_remote_copy(
            part, parts.at[me], part_sem.at[0], part_sem.at[1], device_id={"expert": t}
        ).start()

    for copy in loads[0]:
        copy.wait()
    plan_copy.wait()

    my_move = [plan[layer, me] % slots for layer in range(layers)]

    def units(x):
        return x.reshape(rows // SUB, SUB, LANES)

    def joined(x):
        x = x.reshape(rows // SUB // 2, 2, SUB, cols - full * LANES)
        return jnp.concatenate([x[:, 0], x[:, 1]], axis=-1)

    for i, ref in enumerate((master_0, one_0, two_0, grad.at[0])):
        for c in range(full):
            x = ref[my_move[0], :, c * LANES : (c + 1) * LANES].astype(jnp.float32)
            send_raw[4 * c : 4 * c + 4, i] = units(x)
        x = ref[my_move[0], :, full * LANES :].astype(jnp.float32)
        send_raw[4 * full : 4 * full + 2, i] = joined(x)

    def bytes_of(ref, sem):
        return pltpu.make_async_copy(ref, ref, sem)

    def sized(layer, holder, body):
        short = is_short(layer, holder)

        @pl.when(short)
        def _():
            body(PIECE - 1)

        @pl.when(jnp.logical_not(short))
        def _():
            body(PIECE)

    def post(src, dst, batch, t):
        pltpu.make_async_remote_copy(
            src, dst, out_sem.at[batch, 0], out_sem.at[batch, 1], device_id={"expert": t}
        ).start()

    def out(send, hold, layer, batch):
        for t in targets:

            def start(size):
                src = send.at[pl.ds(offset(layer, t), size)]
                post(src, hold.at[me, pl.ds(0, size)], batch, t)

            sized(layer, t, start)

        def keep(size):
            hold[pl.ds(me, 1), 0:size] = send[pl.ds(offset(layer, me), size)][None]

        sized(layer, me, keep)

    def arrived(hold, layer, batch):
        def wait(size):
            bytes_of(hold.at[0 : GROUP - 1, 0:size], out_sem.at[batch, 1]).wait()

        sized(layer, me, wait)

    def sent(send, layer, batch):
        def wait(size):
            bytes_of(send.at[0 : UNITS - size], out_sem.at[batch, 0]).wait()

        sized(layer, me, wait)

    def reply(src, dst, batch, t):
        pltpu.make_async_remote_copy(
            src, dst, back_sem.at[batch, 0], back_sem.at[batch, 1], device_id={"expert": t}
        ).start()

    def other_whole(body):
        whole = GROUP - sum(is_short(0, holder) for holder in range(GROUP))
        short = is_short(0, me)

        @pl.when(short)
        def _():
            body(whole)

        @pl.when(jnp.logical_not(short))
        def _():
            body(whole - 1)

    for t in near_first:
        post(send_raw.at[pl.ds(offset(0, t), RAW)], hold_raw.at[me], 0, t)
    hold_raw[pl.ds(me, 1)] = send_raw[pl.ds(offset(0, me), RAW)][None]
    for copy in loads[1]:
        copy.wait()

    for c in range(full):
        x = master_1[my_move[1], :, c * LANES : (c + 1) * LANES]
        send_master[4 * c : 4 * c + 4] = units(x)
    send_master[4 * full : 4 * full + 2] = joined(master_1[my_move[1], :, full * LANES :])
    out(send_master, hold_master, 1, 1)

    bytes_of(parts.at[0 : GROUP - 1], part_sem.at[1]).wait()
    line[...] = jnp.sum(parts[...].reshape(GROUP, LANES), axis=0, keepdims=True)
    lines[pl.ds(dp, 1)] = line[...].reshape(1, 1, LANES)
    for d in range(1, DP):
        pltpu.make_async_remote_copy(
            line, lines.at[dp], part_sem.at[2], part_sem.at[3], device_id={"dp": (dp + d) % DP}
        ).start()
    bytes_of(lines.at[0 : DP - 1], part_sem.at[3]).wait()
    total = jnp.sum(lines[...].reshape(DP, LANES), axis=0, keepdims=True)
    total = jnp.sum(total, axis=1, keepdims=True)
    scale = jnp.minimum(1.0, CLIP_RMS * math.sqrt(entry_count) / (jnp.sqrt(total) + 1e-06))

    for holder in range(GROUP):
        if not is_short(0, holder):
            x = send_raw[offset(0, holder) + RAW]
            for i, y in enumerate(adam(x[0], x[1], x[2], x[3], scale)):
                send_rest[holder, i] = y
    for t in targets:

        @pl.when(jnp.logical_not(is_short(0, t)))
        def _():
            post(send_rest.at[t], hold_rest.at[me], 2, t)

    hold_rest[pl.ds(me, 1)] = send_rest[pl.ds(me, 1)]

    def inputs(layer, at):
        return (
            master[layer][at],
            one[layer][at],
            two[layer][at],
            grad[(layer, *at)].astype(jnp.float32),
        )

    for c in range(full):
        at = (my_move[1], slice(None), slice(c * LANES, (c + 1) * LANES))
        for i, x in enumerate(moments(*inputs(1, at)[1:], scale)):
            send_new[4 * c : 4 * c + 4, i] = units(x)
    at = (my_move[1], slice(None), slice(full * LANES, cols))
    for i, x in enumerate(moments(*inputs(1, at)[1:], scale)):
        send_new[4 * full : 4 * full + 2, i] = joined(x)
    out(send_new, hold_new, 1, 3)

    bytes_of(hold_raw.at[0 : GROUP - 1], out_sem.at[0, 1]).wait()

    def forward_raw(t, _):
        source = plan[0, t] // slots
        x = hold_raw[source]
        for i, y in enumerate(adam(x[:, 0], x[:, 1], x[:, 2], x[:, 3], scale)):
            back_0[t, :, i] = y
        return 0

    lax.fori_loop(0, GROUP, forward_raw, 0)
    here = pl.ds(offset(0, me), RAW)
    for t in targets:
        reply(back_0.at[t], home_0.at[here], 0, t)
    home_0[here] = back_0[me]

    for layer in range(layers):

        def resident(slot, _):
            for lo in range(0, cols, 2 * LANES):
                at = (slot, slice(None), slice(lo, min(lo + 2 * LANES, cols)))
                for ref, x in zip((new_w, new_one, new_two), adam(*inputs(layer, at), scale)):
                    ref[(layer, *at)] = x
            return 0

        lax.fori_loop(0, slots, resident, 0)

    @pl.when(jnp.logical_not(is_short(0, me)))
    def _():
        bytes_of(hold_rest.at[0 : GROUP - 1], out_sem.at[2, 1]).wait()

        def forward_rest(t, _):
            back_rest[t] = hold_rest[plan[0, t] // slots]
            return 0

        lax.fori_loop(0, GROUP, forward_rest, 0)
        for t in targets:
            reply(back_rest.at[t], home_0.at[offset(0, me) + RAW], 1, t)
        home_0[pl.ds(offset(0, me) + RAW, 1)] = back_rest[pl.ds(me, 1)]

    arrived(hold_master, 1, 1)
    arrived(hold_new, 1, 3)

    def forward_new(t, _):
        source = plan[1, t] // slots
        x = hold_new[source]
        back_1[t, :, 0] = stepped(hold_master[source], x[:, 0], x[:, 1])
        back_1[t, :, 1:3] = x
        return 0

    lax.fori_loop(0, GROUP, forward_new, 0)

    def send_back(size):
        at = pl.ds(offset(1, me), size)
        for t in targets:
            reply(back_1.at[t, pl.ds(0, size)], home_1.at[at], 2, t)
        home_1[at] = back_1[me, 0:size]

    sized(1, me, send_back)

    bytes_of(home_0.at[0 : RAW * (GROUP - 1)], back_sem.at[0, 1]).wait()
    other_whole(lambda count: bytes_of(home_0.at[0:count], back_sem.at[1, 1]).wait())
    unpack(home_0, landed)
    sized(1, me, lambda size: bytes_of(home_1.at[0 : UNITS - size], back_sem.at[2, 1]).wait())

    bytes_of(parts.at[0 : GROUP - 1], part_sem.at[0]).wait()
    bytes_of(lines.at[0 : DP - 1], part_sem.at[2]).wait()
    bytes_of(send_raw.at[0 : RAW * (GROUP - 1)], out_sem.at[0, 0]).wait()
    sent(send_master, 1, 1)
    other_whole(lambda count: bytes_of(send_rest.at[0:count], out_sem.at[2, 0]).wait())
    sent(send_new, 1, 3)
    bytes_of(back_0.at[0 : GROUP - 1], back_sem.at[0, 0]).wait()

    @pl.when(jnp.logical_not(is_short(0, me)))
    def _():
        bytes_of(back_rest.at[0 : GROUP - 1], back_sem.at[1, 0]).wait()

    sized(
        1, me, lambda size: bytes_of(back_1.at[0 : GROUP - 1, 0:size], back_sem.at[2, 0]).wait()
    )


def exchange(master, moment_one, moment_two, gradient, old_slot, new_slot, entry_count):
    layers, slots, rows, cols = master.shape
    vmem = pl.BlockSpec(memory_space=pltpu.VMEM)
    f32 = jnp.float32
    dma = pltpu.SemaphoreType.DMA
    return pl.pallas_call(
        functools.partial(exchange_kernel, entry_count),
        out_shape=[jax.ShapeDtypeStruct(master.shape, f32)] * 3
        + [
            jax.ShapeDtypeStruct((3, rows, cols), f32),
            jax.ShapeDtypeStruct((UNITS, 3, SUB, LANES), f32),
            jax.ShapeDtypeStruct((layers, GROUP), jnp.int32),
        ],
        in_specs=[pl.BlockSpec(memory_space=pltpu.HBM)] * 6,
        out_specs=[vmem] * 6,
        scratch_shapes=[
            pltpu.VMEM(old_slot.shape, jnp.int32),
            pltpu.VMEM(new_slot.shape, jnp.int32),
            pltpu.SMEM((layers, GROUP), jnp.int32),
            *[pltpu.VMEM(master.shape[1:], f32)] * (3 * layers),
            pltpu.VMEM(master.shape, jnp.bfloat16),
            pltpu.VMEM((UNITS, 4, SUB, LANES), f32),
            pltpu.VMEM((UNITS, SUB, LANES), f32),
            pltpu.VMEM((GROUP, 3, SUB, LANES), f32),
            pltpu.VMEM((UNITS, 2, SUB, LANES), f32),
            pltpu.VMEM((GROUP, RAW, 4, SUB, LANES), f32),
            pltpu.VMEM((GROUP, PIECE, SUB, LANES), f32),
            pltpu.VMEM((GROUP, 3, SUB, LANES), f32),
            pltpu.VMEM((GROUP, PIECE, 2, SUB, LANES), f32),
            pltpu.VMEM((GROUP, RAW, 3, SUB, LANES), f32),
            pltpu.VMEM((GROUP, 3, SUB, LANES), f32),
            pltpu.VMEM((GROUP, PIECE, 3, SUB, LANES), f32),
            pltpu.VMEM((UNITS, 3, SUB, LANES), f32),
            pltpu.VMEM((1, LANES), f32),
            pltpu.VMEM((GROUP, 1, LANES), f32),
            pltpu.VMEM((1, LANES), f32),
            pltpu.VMEM((DP, 1, LANES), f32),
            dma((10,)),
            dma((4,)),
            dma((4, 2)),
            dma((3, 2)),
        ],
        compiler_params=pltpu.CompilerParams(
            collective_id=0, has_side_effects=True, vmem_limit_bytes=40 * 1024 * 1024
        ),
        name="exchange",
    )(
        *(
            pltpu.with_memory_space_constraint(x, pltpu.HBM)
            for x in (master, moment_one, moment_two, gradient, old_slot, new_slot)
        )
    )


def place_kernel(plan, w, one, two, landed, home, out_w, out_one, out_two, last, sem):
    layers, slots = w.shape[:2]
    pairs = ((w, out_w), (one, out_one), (two, out_two))
    mine = lax.broadcasted_iota(jnp.int32, plan.shape, 1) == lax.axis_index("expert")
    chosen = jnp.where(mine, plan[...], 0)
    moved = [jnp.sum(chosen[layer : layer + 1]) % slots for layer in range(layers)]
    for layer in range(layers):
        for i, (src, dst) in enumerate(pairs):
            for slot in range(slots):

                @pl.when(slot != moved[layer])
                def _():
                    pltpu.make_async_copy(
                        src.at[layer, slot], dst.at[layer, slot], sem.at[i]
                    ).start()

    unpack(home, last)
    for layer, block in enumerate((landed, last)):
        for i, (_, dst) in enumerate(pairs):
            pltpu.make_async_copy(block.at[i], dst.at[layer, moved[layer]], sem.at[i]).start()
    for i, (src, dst) in enumerate(pairs):
        pltpu.make_async_copy(src, dst, sem.at[i]).wait()


def place(plan, w, one, two, landed, home):
    rows, cols = w.shape[2:]
    vmem = pl.BlockSpec(memory_space=pltpu.VMEM)
    free = pl.BlockSpec(memory_space=pl.ANY)
    return pl.pallas_call(
        place_kernel,
        out_shape=[jax.ShapeDtypeStruct(w.shape, w.dtype)] * 3,
        in_specs=[vmem] + [free] * 4 + [vmem],
        out_specs=[free] * 3,
        scratch_shapes=[pltpu.VMEM((3, rows, cols), w.dtype), pltpu.SemaphoreType.DMA((3,))],
        compiler_params=pltpu.CompilerParams(vmem_limit_bytes=4 * 1024 * 1024),
        name="place",
    )(plan, w, one, two, landed, home)


def shards(master, moment_one, moment_two, gradient, old_slot, new_slot):
    layers, slots, rows, cols = master.shape
    entry_count = layers * slots * GROUP * rows * DP * cols
    w, one, two, landed, home, plan = exchange(
        master, moment_one, moment_two, gradient, old_slot, new_slot, entry_count
    )
    return place(plan, w, one, two, landed, home)


def solution(mesh):
    spec = P(None, "expert", "dp", None)
    return jax.shard_map(
        shards,
        mesh=mesh,
        in_specs=(spec, spec, spec, spec, P(), P()),
        out_specs=(spec, spec, spec),
        check_vma=False,
    )
```

```python
import functools
import math

import jax
import jax.numpy as jnp
from jax import lax
from jax.experimental import pallas as pl
from jax.experimental.pallas import tpu as pltpu
from jax.sharding import PartitionSpec as P

BETA_ONE = 0.9
BETA_TWO = 0.95
LEARN_RATE = 0.05
DECAY_RATE = 0.1
ADAM_EPS = 1e-08
CLIP_RMS = 2.0
FIRST_FIX = 1.0 - 0.9**10
SECOND_FIX = 1.0 - 0.95**10

ZDIM, YDIM, CORES = 4, 4, 2
GROUP = ZDIM * YDIM * CORES
DP = 4
LANES = 128
SUB = 4
PIECE = 3
RAW = 2
UNITS = 90
BATCH = 8
CHAINS = 6


def move_order():
    moves = [
        (dz, dy, dc)
        for dz in (0, 1, 2, -1)
        for dy in (0, 1, 2, -1)
        for dc in (0, 1)
        if (dz, dy, dc) != (0, 0, 0)
    ]
    neg = lambda v: v if v == 2 else -v
    order = []
    for dz, dy, dc in sorted(moves, key=lambda m: -(abs(m[0]) + abs(m[1]))):
        for m in ((dz, dy, dc), (neg(dz), neg(dy), dc), (dy, dz, dc), (neg(dy), neg(dz), dc)):
            if m not in order:
                order.append(m)
    return order


MOVES = move_order()


def shifted(me, move):
    dz, dy, dc = move
    core, y, z = me % CORES, (me // CORES) % YDIM, me // (CORES * YDIM)
    z = (z + dz + ZDIM) % ZDIM
    y = (y + dy + YDIM) % YDIM
    return (z * YDIM + y) * CORES + (core + dc) % CORES


def moments(moment_one, moment_two, gradient, scale):
    scaled = gradient * scale
    first = BETA_ONE * moment_one + (1.0 - BETA_ONE) * scaled
    second = BETA_TWO * moment_two + (1.0 - BETA_TWO) * scaled * scaled
    return first, second


def stepped(master, first, second):
    step = (first * (1.0 / FIRST_FIX)) / (jnp.sqrt(second * (1.0 / SECOND_FIX)) + ADAM_EPS)
    return master - LEARN_RATE * (step + DECAY_RATE * master)


def adam(master, moment_one, moment_two, gradient, scale):
    first, second = moments(moment_one, moment_two, gradient, scale)
    return stepped(master, first, second), first, second


def is_short(layer, holder):
    return holder % 5 == (4, 2)[layer]


def offset(layer, holder):
    return PIECE * holder - (holder + (0, 2)[layer]) // 5


def unpack(home, block):
    _, rows, cols = block.shape
    full = cols // LANES
    width = cols - full * LANES
    for i in range(block.shape[0]):
        for c in range(full):
            x = home[4 * c : 4 * c + 4, i]
            block[i, :, c * LANES : (c + 1) * LANES] = x.reshape(rows, LANES)
        x = home[4 * full : 4 * full + 2, i]
        x = jnp.stack([x[:, :, :width], x[:, :, width:]], axis=1)
        block[i, :, full * LANES :] = x.reshape(rows, width)


def exchange_kernel(
    entry_count,
    master_hbm,
    one_hbm,
    two_hbm,
    grad_hbm,
    old_hbm,
    new_hbm,
    new_w,
    new_one,
    new_two,
    landed,
    home_1,
    plan_rows,
    old,
    new,
    plan,
    master_0,
    master_1,
    one_0,
    one_1,
    two_0,
    two_1,
    grad,
    send_raw,
    send_master,
    send_rest,
    send_new,
    hold_raw,
    hold_master,
    hold_rest,
    hold_new,
    back_0,
    back_rest,
    back_1,
    home_0,
    part,
    parts,
    line,
    lines,
    load_sem,
    part_sem,
    out_sem,
    back_sem,
):
    layers, slots, rows, cols = master_hbm.shape
    master, one, two = (master_0, master_1), (one_0, one_1), (two_0, two_1)
    full = cols // LANES
    dp = lax.axis_index("dp")
    me = lax.axis_index("expert")
    targets = [shifted(me, m) for m in MOVES]
    near_first = targets[-9:-1] + targets[:-9] + targets[-1:]

    barrier = pltpu.get_barrier_semaphore()
    for t in targets:
        pl.semaphore_signal(barrier, inc=1, device_id={"expert": t})
    for d in range(1, DP):
        pl.semaphore_signal(barrier, inc=1, device_id={"dp": (dp + d) % DP})

    def load(src, dst, sem):
        copy = pltpu.make_async_copy(src, dst, load_sem.at[sem])
        copy.start()
        return copy

    old_load, new_load = load(old_hbm, old, 0), load(new_hbm, new, 1)
    grad_load = load(grad_hbm, grad, 2)
    arrays = ((master_hbm, master), (one_hbm, one), (two_hbm, two))
    def load_layer(layer):
        return [load(src.at[layer], dst[layer], 3 + 3 * layer + i) for i, (src, dst) in enumerate(arrays)]

    loads = [load_layer(0)]

    old_load.wait()
    new_load.wait()
    here = lax.broadcasted_iota(jnp.int32, (GROUP, GROUP * slots), 0)
    diagonal = lax.broadcasted_iota(jnp.int32, (GROUP, GROUP), 0) == lax.broadcasted_iota(
        jnp.int32, (GROUP, GROUP), 1
    )
    for layer in range(layers):
        was, now = old[layer : layer + 1], new[layer : layer + 1]
        word = jnp.where(was != now, (was // slots) * slots + now % slots, 0)
        word = jnp.where(now // slots == here, word, 0)
        word = jnp.sum(word, axis=1, keepdims=True)
        plan_rows[layer : layer + 1] = jnp.sum(jnp.where(diagonal, word, 0), axis=0, keepdims=True)
    plan_copy = pltpu.make_async_copy(plan_rows, plan, load_sem.at[9])
    plan_copy.start()

    grad_load.wait()

    def square(i, accs):
        accs = list(accs)
        for c in range(full):
            g = grad[i // slots, i % slots, :, c * LANES : (c + 1) * LANES].astype(jnp.float32)
            accs[c % CHAINS] += g * g
        return tuple(accs)

    zero = jnp.zeros((rows, LANES), jnp.float32)
    acc = sum(lax.fori_loop(0, layers * slots, square, (zero,) * CHAINS))
    tail = grad[:, :, :, full * LANES :].astype(jnp.float32)
    tail = jnp.sum((tail * tail).reshape(layers * slots * rows, cols - full * LANES), axis=0, keepdims=True)
    acc = jnp.sum(acc, axis=0, keepdims=True)
    part[...] = acc + jnp.concatenate([tail, jnp.zeros_like(tail)], axis=1)
    parts[pl.ds(me, 1)] = part[...].reshape(1, 1, LANES)

    loads.append(load_layer(1))
    pl.semaphore_wait(barrier, len(MOVES) + DP - 1)

    for t in targets:
        pltpu.make_async_remote_copy(
            part, parts.at[me], part_sem.at[0], part_sem.at[1], device_id={"expert": t}
        ).start()

    for copy in loads[0]:
        copy.wait()
    plan_copy.wait()

    my_move = [plan[layer, me] % slots for layer in range(layers)]

    def units(x):
        return x.reshape(rows // SUB, SUB, LANES)

    def joined(x):
        x = x.reshape(rows // SUB // 2, 2, SUB, cols - full * LANES)
        return jnp.concatenate([x[:, 0], x[:, 1]], axis=-1)

    for i, ref in enumerate((master_0, one_0, two_0, grad.at[0])):
        for c in range(full):
            x = ref[my_move[0], :, c * LANES : (c + 1) * LANES].astype(jnp.float32)
            send_raw[4 * c : 4 * c + 4, i] = units(x)
        x = ref[my_move[0], :, full * LANES :].astype(jnp.float32)
        send_raw[4 * full : 4 * full + 2, i] = joined(x)

    def bytes_of(ref, sem):
        return pltpu.make_async_copy(ref, ref, sem)

    def sized(layer, holder, body):
        short = is_short(layer, holder)

        @pl.when(short)
        def _():
            body(PIECE - 1)

        @pl.when(jnp.logical_not(short))
        def _():
            body(PIECE)

    def post(src, dst, batch, t):
        pltpu.make_async_remote_copy(
            src, dst, out_sem.at[batch, 0], out_sem.at[batch, 1], device_id={"expert": t}
        ).start()

    def out(send, hold, layer, batch):
        for t in targets:

            def start(size):
                src = send.at[pl.ds(offset(layer, t), size)]
                post(src, hold.at[me, pl.ds(0, size)], batch, t)

            sized(layer, t, start)

        def keep(size):
            hold[pl.ds(me, 1), 0:size] = send[pl.ds(offset(layer, me), size)][None]

        sized(layer, me, keep)

    def arrived(hold, layer, batch):
        def wait(size):
            bytes_of(hold.at[0 : GROUP - 1, 0:size], out_sem.at[batch, 1]).wait()

        sized(layer, me, wait)

    def sent(send, layer, batch):
        def wait(size):
            bytes_of(send.at[0 : UNITS - size], out_sem.at[batch, 0]).wait()

        sized(layer, me, wait)

    def reply(src, dst, batch, t):
        pltpu.make_async_remote_copy(
            src, dst, back_sem.at[batch, 0], back_sem.at[batch, 1], device_id={"expert": t}
        ).start()

    def other_whole(body):
        whole = GROUP - sum(is_short(0, holder) for holder in range(GROUP))
        short = is_short(0, me)

        @pl.when(short)
        def _():
            body(whole)

        @pl.when(jnp.logical_not(short))
        def _():
            body(whole - 1)

    for t in near_first:
        post(send_raw.at[pl.ds(offset(0, t), RAW)], hold_raw.at[me], 0, t)
    hold_raw[pl.ds(me, 1)] = send_raw[pl.ds(offset(0, me), RAW)][None]
    for copy in loads[1]:
        copy.wait()

    for c in range(full):
        x = master_1[my_move[1], :, c * LANES : (c + 1) * LANES]
        send_master[4 * c : 4 * c + 4] = units(x)
    send_master[4 * full : 4 * full + 2] = joined(master_1[my_move[1], :, full * LANES :])
    out(send_master, hold_master, 1, 1)

    bytes_of(parts.at[0 : GROUP - 1], part_sem.at[1]).wait()
    line[...] = jnp.sum(parts[...].reshape(GROUP, LANES), axis=0, keepdims=True)
    lines[pl.ds(dp, 1)] = line[...].reshape(1, 1, LANES)
    for d in range(1, DP):
        pltpu.make_async_remote_copy(
            line, lines.at[dp], part_sem.at[2], part_sem.at[3], device_id={"dp": (dp + d) % DP}
        ).start()
    bytes_of(lines.at[0 : DP - 1], part_sem.at[3]).wait()
    total = jnp.sum(lines[...].reshape(DP, LANES), axis=0, keepdims=True)
    total = jnp.sum(total, axis=1, keepdims=True)
    scale = jnp.minimum(1.0, CLIP_RMS * math.sqrt(entry_count) / (jnp.sqrt(total) + 1e-06))

    for holder in range(GROUP):
        if not is_short(0, holder):
            x = send_raw[offset(0, holder) + RAW]
            for i, y in enumerate(adam(x[0], x[1], x[2], x[3], scale)):
                send_rest[holder, i] = y
    for t in targets:

        @pl.when(jnp.logical_not(is_short(0, t)))
        def _():
            post(send_rest.at[t], hold_rest.at[me], 2, t)

    hold_rest[pl.ds(me, 1)] = send_rest[pl.ds(me, 1)]

    def inputs(layer, at):
        return (
            master[layer][at],
            one[layer][at],
            two[layer][at],
            grad[(layer, *at)].astype(jnp.float32),
        )

    for c in range(full):
        at = (my_move[1], slice(None), slice(c * LANES, (c + 1) * LANES))
        for i, x in enumerate(moments(*inputs(1, at)[1:], scale)):
            send_new[4 * c : 4 * c + 4, i] = units(x)
    at = (my_move[1], slice(None), slice(full * LANES, cols))
    for i, x in enumerate(moments(*inputs(1, at)[1:], scale)):
        send_new[4 * full : 4 * full + 2, i] = joined(x)
    out(send_new, hold_new, 1, 3)

    bytes_of(hold_raw.at[0 : GROUP - 1], out_sem.at[0, 1]).wait()

    def forward_raw(t, _):
        source = plan[0, t] // slots
        x = hold_raw[source]
        for i, y in enumerate(adam(x[:, 0], x[:, 1], x[:, 2], x[:, 3], scale)):
            back_0[t, :, i] = y
        return 0

    lax.fori_loop(0, GROUP, forward_raw, 0)
    here = pl.ds(offset(0, me), RAW)
    for t in targets:
        reply(back_0.at[t], home_0.at[here], 0, t)
    home_0[here] = back_0[me]

    @pl.when(jnp.logical_not(is_short(0, me)))
    def _():
        bytes_of(hold_rest.at[0 : GROUP - 1], out_sem.at[2, 1]).wait()

        def forward_rest(t, _):
            back_rest[t] = hold_rest[plan[0, t] // slots]
            return 0

        lax.fori_loop(0, GROUP, forward_rest, 0)
        for t in targets:
            reply(back_rest.at[t], home_0.at[offset(0, me) + RAW], 1, t)
        home_0[pl.ds(offset(0, me) + RAW, 1)] = back_rest[pl.ds(me, 1)]

    arrived(hold_master, 1, 1)
    arrived(hold_new, 1, 3)

    def forward_new(t):
        source = plan[1, t] // slots
        x = hold_new[source]
        back_1[t, :, 0] = stepped(hold_master[source], x[:, 0], x[:, 1])
        back_1[t, :, 1:3] = x

    def send_back(some):
        def start(size):
            for t in some:
                src = back_1.at[t, pl.ds(0, size)]
                reply(src, home_1.at[pl.ds(offset(1, me), size)], 2, t)

        sized(1, me, start)

    groups = [targets[k : k + BATCH] for k in range(0, len(targets), BATCH)]
    for some, before in zip(groups + [[me]], [[]] + groups):
        for t in some:
            forward_new(t)
        send_back(before)

    def keep_back(size):
        home_1[pl.ds(offset(1, me), size)] = back_1[me, 0:size]

    sized(1, me, keep_back)

    for layer in range(layers):

        def resident(slot, _):
            for lo in range(0, cols, 2 * LANES):
                at = (slot, slice(None), slice(lo, min(lo + 2 * LANES, cols)))
                for ref, x in zip((new_w, new_one, new_two), adam(*inputs(layer, at), scale)):
                    ref[(layer, *at)] = x
            return 0

        lax.fori_loop(0, slots, resident, 0)

    bytes_of(home_0.at[0 : RAW * (GROUP - 1)], back_sem.at[0, 1]).wait()
    other_whole(lambda count: bytes_of(home_0.at[0:count], back_sem.at[1, 1]).wait())
    unpack(home_0, landed)
    sized(1, me, lambda size: bytes_of(home_1.at[0 : UNITS - size], back_sem.at[2, 1]).wait())

    bytes_of(parts.at[0 : GROUP - 1], part_sem.at[0]).wait()
    bytes_of(lines.at[0 : DP - 1], part_sem.at[2]).wait()
    bytes_of(send_raw.at[0 : RAW * (GROUP - 1)], out_sem.at[0, 0]).wait()
    sent(send_master, 1, 1)
    other_whole(lambda count: bytes_of(send_rest.at[0:count], out_sem.at[2, 0]).wait())
    sent(send_new, 1, 3)
    bytes_of(back_0.at[0 : GROUP - 1], back_sem.at[0, 0]).wait()

    @pl.when(jnp.logical_not(is_short(0, me)))
    def _():
        bytes_of(back_rest.at[0 : GROUP - 1], back_sem.at[1, 0]).wait()

    sized(
        1, me, lambda size: bytes_of(back_1.at[0 : GROUP - 1, 0:size], back_sem.at[2, 0]).wait()
    )


def exchange(master, moment_one, moment_two, gradient, old_slot, new_slot, entry_count):
    layers, slots, rows, cols = master.shape
    vmem = pl.BlockSpec(memory_space=pltpu.VMEM)
    f32 = jnp.float32
    dma = pltpu.SemaphoreType.DMA
    return pl.pallas_call(
        functools.partial(exchange_kernel, entry_count),
        out_shape=[jax.ShapeDtypeStruct(master.shape, f32)] * 3
        + [
            jax.ShapeDtypeStruct((3, rows, cols), f32),
            jax.ShapeDtypeStruct((UNITS, 3, SUB, LANES), f32),
            jax.ShapeDtypeStruct((layers, GROUP), jnp.int32),
        ],
        in_specs=[pl.BlockSpec(memory_space=pltpu.HBM)] * 6,
        out_specs=[vmem] * 6,
        scratch_shapes=[
            pltpu.VMEM(old_slot.shape, jnp.int32),
            pltpu.VMEM(new_slot.shape, jnp.int32),
            pltpu.SMEM((layers, GROUP), jnp.int32),
            *[pltpu.VMEM(master.shape[1:], f32)] * (3 * layers),
            pltpu.VMEM(master.shape, jnp.bfloat16),
            pltpu.VMEM((UNITS, 4, SUB, LANES), f32),
            pltpu.VMEM((UNITS, SUB, LANES), f32),
            pltpu.VMEM((GROUP, 3, SUB, LANES), f32),
            pltpu.VMEM((UNITS, 2, SUB, LANES), f32),
            pltpu.VMEM((GROUP, RAW, 4, SUB, LANES), f32),
            pltpu.VMEM((GROUP, PIECE, SUB, LANES), f32),
            pltpu.VMEM((GROUP, 3, SUB, LANES), f32),
            pltpu.VMEM((GROUP, PIECE, 2, SUB, LANES), f32),
            pltpu.VMEM((GROUP, RAW, 3, SUB, LANES), f32),
            pltpu.VMEM((GROUP, 3, SUB, LANES), f32),
            pltpu.VMEM((GROUP, PIECE, 3, SUB, LANES), f32),
            pltpu.VMEM((UNITS, 3, SUB, LANES), f32),
            pltpu.VMEM((1, LANES), f32),
            pltpu.VMEM((GROUP, 1, LANES), f32),
            pltpu.VMEM((1, LANES), f32),
            pltpu.VMEM((DP, 1, LANES), f32),
            dma((10,)),
            dma((4,)),
            dma((4, 2)),
            dma((3, 2)),
        ],
        compiler_params=pltpu.CompilerParams(
            collective_id=0, has_side_effects=True, vmem_limit_bytes=40 * 1024 * 1024
        ),
        name="exchange",
    )(
        *(
            pltpu.with_memory_space_constraint(x, pltpu.HBM)
            for x in (master, moment_one, moment_two, gradient, old_slot, new_slot)
        )
    )


def place_kernel(plan, w, one, two, landed, home, out_w, out_one, out_two, last, sem):
    layers, slots = w.shape[:2]
    pairs = ((w, out_w), (one, out_one), (two, out_two))
    mine = lax.broadcasted_iota(jnp.int32, plan.shape, 1) == lax.axis_index("expert")
    chosen = jnp.where(mine, plan[...], 0)
    moved = [jnp.sum(chosen[layer : layer + 1]) % slots for layer in range(layers)]
    for layer in range(layers):
        for i, (src, dst) in enumerate(pairs):
            for slot in range(slots):

                @pl.when(slot != moved[layer])
                def _():
                    pltpu.make_async_copy(
                        src.at[layer, slot], dst.at[layer, slot], sem.at[i]
                    ).start()

    unpack(home, last)
    for layer, block in enumerate((landed, last)):
        for i, (_, dst) in enumerate(pairs):
            pltpu.make_async_copy(block.at[i], dst.at[layer, moved[layer]], sem.at[i]).start()
    for i, (src, dst) in enumerate(pairs):
        pltpu.make_async_copy(src, dst, sem.at[i]).wait()


def place(plan, w, one, two, landed, home):
    rows, cols = w.shape[2:]
    vmem = pl.BlockSpec(memory_space=pltpu.VMEM)
    free = pl.BlockSpec(memory_space=pl.ANY)
    return pl.pallas_call(
        place_kernel,
        out_shape=[jax.ShapeDtypeStruct(w.shape, w.dtype)] * 3,
        in_specs=[vmem] + [free] * 4 + [vmem],
        out_specs=[free] * 3,
        scratch_shapes=[pltpu.VMEM((3, rows, cols), w.dtype), pltpu.SemaphoreType.DMA((3,))],
        compiler_params=pltpu.CompilerParams(vmem_limit_bytes=4 * 1024 * 1024),
        name="place",
    )(plan, w, one, two, landed, home)


def shards(master, moment_one, moment_two, gradient, old_slot, new_slot):
    layers, slots, rows, cols = master.shape
    entry_count = layers * slots * GROUP * rows * DP * cols
    w, one, two, landed, home, plan = exchange(
        master, moment_one, moment_two, gradient, old_slot, new_slot, entry_count
    )
    return place(plan, w, one, two, landed, home)


def solution(mesh):
    spec = P(None, "expert", "dp", None)
    return jax.shard_map(
        shards,
        mesh=mesh,
        in_specs=(spec, spec, spec, spec, P(), P()),
        out_specs=(spec, spec, spec),
        check_vma=False,
    )
```

```python
import functools
import math

import jax
import jax.numpy as jnp
from jax import lax
from jax.experimental import pallas as pl
from jax.experimental.pallas import tpu as pltpu
from jax.sharding import PartitionSpec as P

BETA_ONE = 0.9
BETA_TWO = 0.95
LEARN_RATE = 0.05
DECAY_RATE = 0.1
ADAM_EPS = 1e-08
CLIP_RMS = 2.0
FIRST_FIX = 1.0 - 0.9**10
SECOND_FIX = 1.0 - 0.95**10

ZDIM, YDIM, CORES = 4, 4, 2
GROUP = ZDIM * YDIM * CORES
DP = 4
LANES = 128
SUB = 4
PIECE = 3
RAW = 2
UNITS = 90
BATCH = 8
CHAINS = 6


def move_order():
    moves = [
        (dz, dy, dc)
        for dz in (0, 1, 2, -1)
        for dy in (0, 1, 2, -1)
        for dc in (0, 1)
        if (dz, dy, dc) != (0, 0, 0)
    ]
    neg = lambda v: v if v == 2 else -v
    order = []
    for dz, dy, dc in sorted(moves, key=lambda m: -(abs(m[0]) + abs(m[1]))):
        for m in ((dz, dy, dc), (neg(dz), neg(dy), dc), (dy, dz, dc), (neg(dy), neg(dz), dc)):
            if m not in order:
                order.append(m)
    return order


MOVES = move_order()


def shifted(me, move):
    dz, dy, dc = move
    core, y, z = me % CORES, (me // CORES) % YDIM, me // (CORES * YDIM)
    z = (z + dz + ZDIM) % ZDIM
    y = (y + dy + YDIM) % YDIM
    return (z * YDIM + y) * CORES + (core + dc) % CORES


def moments(moment_one, moment_two, gradient, scale):
    scaled = gradient * scale
    first = BETA_ONE * moment_one + (1.0 - BETA_ONE) * scaled
    second = BETA_TWO * moment_two + (1.0 - BETA_TWO) * scaled * scaled
    return first, second


def stepped(master, first, second):
    step = (first * (1.0 / FIRST_FIX)) / (jnp.sqrt(second * (1.0 / SECOND_FIX)) + ADAM_EPS)
    return master - LEARN_RATE * (step + DECAY_RATE * master)


def adam(master, moment_one, moment_two, gradient, scale):
    first, second = moments(moment_one, moment_two, gradient, scale)
    return stepped(master, first, second), first, second


def is_short(layer, holder):
    return holder % 5 == (4, 2)[layer]


def offset(layer, holder):
    return PIECE * holder - (holder + (0, 2)[layer]) // 5


def unpack(home, block):
    _, rows, cols = block.shape
    full = cols // LANES
    width = cols - full * LANES
    for i in range(block.shape[0]):
        for c in range(full):
            x = home[4 * c : 4 * c + 4, i]
            block[i, :, c * LANES : (c + 1) * LANES] = x.reshape(rows, LANES)
        x = home[4 * full : 4 * full + 2, i]
        x = jnp.stack([x[:, :, :width], x[:, :, width:]], axis=1)
        block[i, :, full * LANES :] = x.reshape(rows, width)


def exchange_kernel(
    entry_count,
    master_hbm,
    one_hbm,
    two_hbm,
    grad_hbm,
    old_hbm,
    new_hbm,
    new_w,
    new_one,
    new_two,
    landed,
    home_1,
    plan_rows,
    old,
    new,
    plan,
    master_0,
    master_1,
    one_0,
    one_1,
    two_0,
    two_1,
    grad,
    send_raw,
    send_master,
    send_rest,
    send_new,
    hold_raw,
    hold_master,
    hold_rest,
    hold_new,
    back_0,
    back_rest,
    back_1,
    home_0,
    part,
    parts,
    line,
    lines,
    load_sem,
    part_sem,
    out_sem,
    back_sem,
):
    layers, slots, rows, cols = master_hbm.shape
    master, one, two = (master_0, master_1), (one_0, one_1), (two_0, two_1)
    full = cols // LANES
    dp = lax.axis_index("dp")
    me = lax.axis_index("expert")
    targets = [shifted(me, m) for m in MOVES]
    near_first = targets[-9:-1] + targets[:-9] + targets[-1:]

    barrier = pltpu.get_barrier_semaphore()
    for t in targets:
        pl.semaphore_signal(barrier, inc=1, device_id={"expert": t})
    for d in range(1, DP):
        pl.semaphore_signal(barrier, inc=1, device_id={"dp": (dp + d) % DP})

    def load(src, dst, sem):
        copy = pltpu.make_async_copy(src, dst, load_sem.at[sem])
        copy.start()
        return copy

    old_load, new_load = load(old_hbm, old, 0), load(new_hbm, new, 1)
    grad_load = load(grad_hbm, grad, 2)
    arrays = ((master_hbm, master), (one_hbm, one), (two_hbm, two))
    def load_layer(layer):
        return [load(src.at[layer], dst[layer], 3 + 3 * layer + i) for i, (src, dst) in enumerate(arrays)]

    loads = [load_layer(0)]

    old_load.wait()
    new_load.wait()
    here = lax.broadcasted_iota(jnp.int32, (GROUP, GROUP * slots), 0)
    diagonal = lax.broadcasted_iota(jnp.int32, (GROUP, GROUP), 0) == lax.broadcasted_iota(
        jnp.int32, (GROUP, GROUP), 1
    )
    for layer in range(layers):
        was, now = old[layer : layer + 1], new[layer : layer + 1]
        word = jnp.where(was != now, (was // slots) * slots + now % slots, 0)
        word = jnp.where(now // slots == here, word, 0)
        word = jnp.sum(word, axis=1, keepdims=True)
        plan_rows[layer : layer + 1] = jnp.sum(jnp.where(diagonal, word, 0), axis=0, keepdims=True)
    plan_copy = pltpu.make_async_copy(plan_rows, plan, load_sem.at[9])
    plan_copy.start()

    grad_load.wait()

    def square(i, accs):
        accs = list(accs)
        for c in range(full):
            g = grad[i // slots, i % slots, :, c * LANES : (c + 1) * LANES].astype(jnp.float32)
            accs[c % CHAINS] += g * g
        return tuple(accs)

    zero = jnp.zeros((rows, LANES), jnp.float32)
    acc = sum(lax.fori_loop(0, layers * slots, square, (zero,) * CHAINS))
    tail = grad[:, :, :, full * LANES :].astype(jnp.float32)
    tail = jnp.sum((tail * tail).reshape(layers * slots * rows, cols - full * LANES), axis=0, keepdims=True)
    acc = jnp.sum(acc, axis=0, keepdims=True)
    part[...] = acc + jnp.concatenate([tail, jnp.zeros_like(tail)], axis=1)
    parts[pl.ds(me, 1)] = part[...].reshape(1, 1, LANES)

    loads.append(load_layer(1))
    pl.semaphore_wait(barrier, len(MOVES) + DP - 1)

    for t in targets:
        pltpu.make_async_remote_copy(
            part, parts.at[me], part_sem.at[0], part_sem.at[1], device_id={"expert": t}
        ).start()

    for copy in loads[0]:
        copy.wait()
    plan_copy.wait()

    my_move = [plan[layer, me] % slots for layer in range(layers)]

    def units(x):
        return x.reshape(rows // SUB, SUB, LANES)

    def joined(x):
        x = x.reshape(rows // SUB // 2, 2, SUB, cols - full * LANES)
        return jnp.concatenate([x[:, 0], x[:, 1]], axis=-1)

    for i, ref in enumerate((master_0, one_0, two_0, grad.at[0])):
        for c in range(full):
            x = ref[my_move[0], :, c * LANES : (c + 1) * LANES].astype(jnp.float32)
            send_raw[4 * c : 4 * c + 4, i] = units(x)
        x = ref[my_move[0], :, full * LANES :].astype(jnp.float32)
        send_raw[4 * full : 4 * full + 2, i] = joined(x)

    def bytes_of(ref, sem):
        return pltpu.make_async_copy(ref, ref, sem)

    def sized(layer, holder, body):
        short = is_short(layer, holder)

        @pl.when(short)
        def _():
            body(PIECE - 1)

        @pl.when(jnp.logical_not(short))
        def _():
            body(PIECE)

    def post(src, dst, batch, t):
        pltpu.make_async_remote_copy(
            src, dst, out_sem.at[batch, 0], out_sem.at[batch, 1], device_id={"expert": t}
        ).start()

    def out(send, hold, layer, batch):
        for t in targets:

            def start(size):
                src = send.at[pl.ds(offset(layer, t), size)]
                post(src, hold.at[me, pl.ds(0, size)], batch, t)

            sized(layer, t, start)

        def keep(size):
            hold[pl.ds(me, 1), 0:size] = send[pl.ds(offset(layer, me), size)][None]

        sized(layer, me, keep)

    def arrived(hold, layer, batch):
        def wait(size):
            bytes_of(hold.at[0 : GROUP - 1, 0:size], out_sem.at[batch, 1]).wait()

        sized(layer, me, wait)

    def sent(send, layer, batch):
        def wait(size):
            bytes_of(send.at[0 : UNITS - size], out_sem.at[batch, 0]).wait()

        sized(layer, me, wait)

    def reply(src, dst, batch, t):
        pltpu.make_async_remote_copy(
            src, dst, back_sem.at[batch, 0], back_sem.at[batch, 1], device_id={"expert": t}
        ).start()

    def other_whole(body):
        whole = GROUP - sum(is_short(0, holder) for holder in range(GROUP))
        short = is_short(0, me)

        @pl.when(short)
        def _():
            body(whole)

        @pl.when(jnp.logical_not(short))
        def _():
            body(whole - 1)

    for t in near_first:
        post(send_raw.at[pl.ds(offset(0, t), RAW)], hold_raw.at[me], 0, t)
    hold_raw[pl.ds(me, 1)] = send_raw[pl.ds(offset(0, me), RAW)][None]
    for copy in loads[1]:
        copy.wait()

    for c in range(full):
        x = master_1[my_move[1], :, c * LANES : (c + 1) * LANES]
        send_master[4 * c : 4 * c + 4] = units(x)
    send_master[4 * full : 4 * full + 2] = joined(master_1[my_move[1], :, full * LANES :])
    out(send_master, hold_master, 1, 1)

    bytes_of(parts.at[0 : GROUP - 1], part_sem.at[1]).wait()
    line[...] = jnp.sum(parts[...].reshape(GROUP, LANES), axis=0, keepdims=True)
    lines[pl.ds(dp, 1)] = line[...].reshape(1, 1, LANES)
    for d in range(1, DP):
        pltpu.make_async_remote_copy(
            line, lines.at[dp], part_sem.at[2], part_sem.at[3], device_id={"dp": (dp + d) % DP}
        ).start()
    bytes_of(lines.at[0 : DP - 1], part_sem.at[3]).wait()
    total = jnp.sum(lines[...].reshape(DP, LANES), axis=0, keepdims=True)
    total = jnp.sum(total, axis=1, keepdims=True)
    scale = jnp.minimum(1.0, CLIP_RMS * math.sqrt(entry_count) / (jnp.sqrt(total) + 1e-06))

    for holder in range(GROUP):
        if not is_short(0, holder):
            x = send_raw[offset(0, holder) + RAW]
            for i, y in enumerate(adam(x[0], x[1], x[2], x[3], scale)):
                send_rest[holder, i] = y
    for t in targets:

        @pl.when(jnp.logical_not(is_short(0, t)))
        def _():
            post(send_rest.at[t], hold_rest.at[me], 2, t)

    hold_rest[pl.ds(me, 1)] = send_rest[pl.ds(me, 1)]

    def inputs(layer, at):
        return (
            master[layer][at],
            one[layer][at],
            two[layer][at],
            grad[(layer, *at)].astype(jnp.float32),
        )

    for c in range(full):
        at = (my_move[1], slice(None), slice(c * LANES, (c + 1) * LANES))
        for i, x in enumerate(moments(*inputs(1, at)[1:], scale)):
            send_new[4 * c : 4 * c + 4, i] = units(x)
    at = (my_move[1], slice(None), slice(full * LANES, cols))
    for i, x in enumerate(moments(*inputs(1, at)[1:], scale)):
        send_new[4 * full : 4 * full + 2, i] = joined(x)
    out(send_new, hold_new, 1, 3)

    bytes_of(hold_raw.at[0 : GROUP - 1], out_sem.at[0, 1]).wait()

    def forward_raw(t):
        x = hold_raw[plan[0, t] // slots]
        for i, y in enumerate(adam(x[:, 0], x[:, 1], x[:, 2], x[:, 3], scale)):
            back_0[t, :, i] = y

    here = pl.ds(offset(0, me), RAW)
    groups = [targets[k : k + BATCH] for k in range(0, len(targets), BATCH)]
    for some, before in zip(groups + [[me]], [[]] + groups):
        for t in some:
            forward_raw(t)
        for t in before:
            reply(back_0.at[t], home_0.at[here], 0, t)
    home_0[here] = back_0[me]

    @pl.when(jnp.logical_not(is_short(0, me)))
    def _():
        bytes_of(hold_rest.at[0 : GROUP - 1], out_sem.at[2, 1]).wait()

        def forward_rest(t, _):
            back_rest[t] = hold_rest[plan[0, t] // slots]
            return 0

        lax.fori_loop(0, GROUP, forward_rest, 0)
        for t in targets:
            reply(back_rest.at[t], home_0.at[offset(0, me) + RAW], 1, t)
        home_0[pl.ds(offset(0, me) + RAW, 1)] = back_rest[pl.ds(me, 1)]

    arrived(hold_master, 1, 1)
    arrived(hold_new, 1, 3)

    def forward_new(t):
        source = plan[1, t] // slots
        x = hold_new[source]
        back_1[t, :, 0] = stepped(hold_master[source], x[:, 0], x[:, 1])
        back_1[t, :, 1:3] = x

    def send_back(some):
        def start(size):
            for t in some:
                src = back_1.at[t, pl.ds(0, size)]
                reply(src, home_1.at[pl.ds(offset(1, me), size)], 2, t)

        sized(1, me, start)

    for some, before in zip(groups + [[me]], [[]] + groups):
        for t in some:
            forward_new(t)
        send_back(before)

    def keep_back(size):
        home_1[pl.ds(offset(1, me), size)] = back_1[me, 0:size]

    sized(1, me, keep_back)

    for layer in range(layers):

        def resident(slot, _):
            for lo in range(0, cols, 2 * LANES):
                at = (slot, slice(None), slice(lo, min(lo + 2 * LANES, cols)))
                for ref, x in zip((new_w, new_one, new_two), adam(*inputs(layer, at), scale)):
                    ref[(layer, *at)] = x
            return 0

        lax.fori_loop(0, slots, resident, 0)

    bytes_of(home_0.at[0 : RAW * (GROUP - 1)], back_sem.at[0, 1]).wait()
    other_whole(lambda count: bytes_of(home_0.at[0:count], back_sem.at[1, 1]).wait())
    unpack(home_0, landed)
    sized(1, me, lambda size: bytes_of(home_1.at[0 : UNITS - size], back_sem.at[2, 1]).wait())

    bytes_of(parts.at[0 : GROUP - 1], part_sem.at[0]).wait()
    bytes_of(lines.at[0 : DP - 1], part_sem.at[2]).wait()
    bytes_of(send_raw.at[0 : RAW * (GROUP - 1)], out_sem.at[0, 0]).wait()
    sent(send_master, 1, 1)
    other_whole(lambda count: bytes_of(send_rest.at[0:count], out_sem.at[2, 0]).wait())
    sent(send_new, 1, 3)
    bytes_of(back_0.at[0 : GROUP - 1], back_sem.at[0, 0]).wait()

    @pl.when(jnp.logical_not(is_short(0, me)))
    def _():
        bytes_of(back_rest.at[0 : GROUP - 1], back_sem.at[1, 0]).wait()

    sized(
        1, me, lambda size: bytes_of(back_1.at[0 : GROUP - 1, 0:size], back_sem.at[2, 0]).wait()
    )


def exchange(master, moment_one, moment_two, gradient, old_slot, new_slot, entry_count):
    layers, slots, rows, cols = master.shape
    vmem = pl.BlockSpec(memory_space=pltpu.VMEM)
    f32 = jnp.float32
    dma = pltpu.SemaphoreType.DMA
    return pl.pallas_call(
        functools.partial(exchange_kernel, entry_count),
        out_shape=[jax.ShapeDtypeStruct(master.shape, f32)] * 3
        + [
            jax.ShapeDtypeStruct((3, rows, cols), f32),
            jax.ShapeDtypeStruct((UNITS, 3, SUB, LANES), f32),
            jax.ShapeDtypeStruct((layers, GROUP), jnp.int32),
        ],
        in_specs=[pl.BlockSpec(memory_space=pltpu.HBM)] * 6,
        out_specs=[vmem] * 6,
        scratch_shapes=[
            pltpu.VMEM(old_slot.shape, jnp.int32),
            pltpu.VMEM(new_slot.shape, jnp.int32),
            pltpu.SMEM((layers, GROUP), jnp.int32),
            *[pltpu.VMEM(master.shape[1:], f32)] * (3 * layers),
            pltpu.VMEM(master.shape, jnp.bfloat16),
            pltpu.VMEM((UNITS, 4, SUB, LANES), f32),
            pltpu.VMEM((UNITS, SUB, LANES), f32),
            pltpu.VMEM((GROUP, 3, SUB, LANES), f32),
            pltpu.VMEM((UNITS, 2, SUB, LANES), f32),
            pltpu.VMEM((GROUP, RAW, 4, SUB, LANES), f32),
            pltpu.VMEM((GROUP, PIECE, SUB, LANES), f32),
            pltpu.VMEM((GROUP, 3, SUB, LANES), f32),
            pltpu.VMEM((GROUP, PIECE, 2, SUB, LANES), f32),
            pltpu.VMEM((GROUP, RAW, 3, SUB, LANES), f32),
            pltpu.VMEM((GROUP, 3, SUB, LANES), f32),
            pltpu.VMEM((GROUP, PIECE, 3, SUB, LANES), f32),
            pltpu.VMEM((UNITS, 3, SUB, LANES), f32),
            pltpu.VMEM((1, LANES), f32),
            pltpu.VMEM((GROUP, 1, LANES), f32),
            pltpu.VMEM((1, LANES), f32),
            pltpu.VMEM((DP, 1, LANES), f32),
            dma((10,)),
            dma((4,)),
            dma((4, 2)),
            dma((3, 2)),
        ],
        compiler_params=pltpu.CompilerParams(
            collective_id=0, has_side_effects=True, vmem_limit_bytes=40 * 1024 * 1024
        ),
        name="exchange",
    )(
        *(
            pltpu.with_memory_space_constraint(x, pltpu.HBM)
            for x in (master, moment_one, moment_two, gradient, old_slot, new_slot)
        )
    )


def place_kernel(plan, w, one, two, landed, home, out_w, out_one, out_two, last, sem):
    layers, slots = w.shape[:2]
    pairs = ((w, out_w), (one, out_one), (two, out_two))
    mine = lax.broadcasted_iota(jnp.int32, plan.shape, 1) == lax.axis_index("expert")
    chosen = jnp.where(mine, plan[...], 0)
    moved = [jnp.sum(chosen[layer : layer + 1]) % slots for layer in range(layers)]
    for layer in range(layers):
        for i, (src, dst) in enumerate(pairs):
            for slot in range(slots):

                @pl.when(slot != moved[layer])
                def _():
                    pltpu.make_async_copy(
                        src.at[layer, slot], dst.at[layer, slot], sem.at[i]
                    ).start()

    unpack(home, last)
    for layer, block in enumerate((landed, last)):
        for i, (_, dst) in enumerate(pairs):
            pltpu.make_async_copy(block.at[i], dst.at[layer, moved[layer]], sem.at[i]).start()
    for i, (src, dst) in enumerate(pairs):
        pltpu.make_async_copy(src, dst, sem.at[i]).wait()


def place(plan, w, one, two, landed, home):
    rows, cols = w.shape[2:]
    vmem = pl.BlockSpec(memory_space=pltpu.VMEM)
    free = pl.BlockSpec(memory_space=pl.ANY)
    return pl.pallas_call(
        place_kernel,
        out_shape=[jax.ShapeDtypeStruct(w.shape, w.dtype)] * 3,
        in_specs=[vmem] + [free] * 4 + [vmem],
        out_specs=[free] * 3,
        scratch_shapes=[pltpu.VMEM((3, rows, cols), w.dtype), pltpu.SemaphoreType.DMA((3,))],
        compiler_params=pltpu.CompilerParams(vmem_limit_bytes=4 * 1024 * 1024),
        name="place",
    )(plan, w, one, two, landed, home)


def shards(master, moment_one, moment_two, gradient, old_slot, new_slot):
    layers, slots, rows, cols = master.shape
    entry_count = layers * slots * GROUP * rows * DP * cols
    w, one, two, landed, home, plan = exchange(
        master, moment_one, moment_two, gradient, old_slot, new_slot, entry_count
    )
    return place(plan, w, one, two, landed, home)


def solution(mesh):
    spec = P(None, "expert", "dp", None)
    return jax.shard_map(
        shards,
        mesh=mesh,
        in_specs=(spec, spec, spec, spec, P(), P()),
        out_specs=(spec, spec, spec),
        check_vma=False,
    )
```

```python
import functools
import math

import jax
import jax.numpy as jnp
from jax import lax
from jax.experimental import pallas as pl
from jax.experimental.pallas import tpu as pltpu
from jax.sharding import PartitionSpec as P

BETA_ONE = 0.9
BETA_TWO = 0.95
LEARN_RATE = 0.05
DECAY_RATE = 0.1
ADAM_EPS = 1e-08
CLIP_RMS = 2.0
FIRST_FIX = 1.0 - 0.9**10
SECOND_FIX = 1.0 - 0.95**10

ZDIM, YDIM, CORES = 4, 4, 2
GROUP = ZDIM * YDIM * CORES
DP = 4
LANES = 128
SUB = 4
PIECE = 3
RAW = 2
UNITS = 90
BATCH = 16
CHAINS = 6


def move_order():
    moves = [
        (dz, dy, dc)
        for dz in (0, 1, 2, -1)
        for dy in (0, 1, 2, -1)
        for dc in (0, 1)
        if (dz, dy, dc) != (0, 0, 0)
    ]
    neg = lambda v: v if v == 2 else -v
    order = []
    for dz, dy, dc in sorted(moves, key=lambda m: -(abs(m[0]) + abs(m[1]))):
        for m in ((dz, dy, dc), (neg(dz), neg(dy), dc), (dy, dz, dc), (neg(dy), neg(dz), dc)):
            if m not in order:
                order.append(m)
    return order


MOVES = move_order()


def shifted(me, move):
    dz, dy, dc = move
    core, y, z = me % CORES, (me // CORES) % YDIM, me // (CORES * YDIM)
    z = (z + dz + ZDIM) % ZDIM
    y = (y + dy + YDIM) % YDIM
    return (z * YDIM + y) * CORES + (core + dc) % CORES


def moments(moment_one, moment_two, gradient, scale):
    scaled = gradient * scale
    first = BETA_ONE * moment_one + (1.0 - BETA_ONE) * scaled
    second = BETA_TWO * moment_two + (1.0 - BETA_TWO) * scaled * scaled
    return first, second


def stepped(master, first, second):
    step = (first * (1.0 / FIRST_FIX)) / (jnp.sqrt(second * (1.0 / SECOND_FIX)) + ADAM_EPS)
    return master - LEARN_RATE * (step + DECAY_RATE * master)


def adam(master, moment_one, moment_two, gradient, scale):
    first, second = moments(moment_one, moment_two, gradient, scale)
    return stepped(master, first, second), first, second


def is_short(layer, holder):
    return holder % 5 == (4, 2)[layer]


def offset(layer, holder):
    return PIECE * holder - (holder + (0, 2)[layer]) // 5


def unpack(home, block):
    _, rows, cols = block.shape
    full = cols // LANES
    width = cols - full * LANES
    for i in range(block.shape[0]):
        for c in range(full):
            x = home[4 * c : 4 * c + 4, i]
            block[i, :, c * LANES : (c + 1) * LANES] = x.reshape(rows, LANES)
        x = home[4 * full : 4 * full + 2, i]
        x = jnp.stack([x[:, :, :width], x[:, :, width:]], axis=1)
        block[i, :, full * LANES :] = x.reshape(rows, width)


def exchange_kernel(
    entry_count,
    master_hbm,
    one_hbm,
    two_hbm,
    grad_hbm,
    old_hbm,
    new_hbm,
    new_w,
    new_one,
    new_two,
    landed,
    home_1,
    plan_rows,
    old,
    new,
    plan,
    master_0,
    master_1,
    one_0,
    one_1,
    two_0,
    two_1,
    grad,
    send_raw,
    send_master,
    send_rest,
    send_new,
    hold_raw,
    hold_master,
    hold_rest,
    hold_new,
    back_0,
    back_rest,
    back_1,
    home_0,
    part,
    parts,
    line,
    lines,
    load_sem,
    part_sem,
    out_sem,
    back_sem,
):
    layers, slots, rows, cols = master_hbm.shape
    master, one, two = (master_0, master_1), (one_0, one_1), (two_0, two_1)
    full = cols // LANES
    dp = lax.axis_index("dp")
    me = lax.axis_index("expert")
    targets = [shifted(me, m) for m in MOVES]
    near_first = targets[-9:-1] + targets[:-9] + targets[-1:]

    barrier = pltpu.get_barrier_semaphore()
    for t in targets:
        pl.semaphore_signal(barrier, inc=1, device_id={"expert": t})
    for d in range(1, DP):
        pl.semaphore_signal(barrier, inc=1, device_id={"dp": (dp + d) % DP})

    def load(src, dst, sem):
        copy = pltpu.make_async_copy(src, dst, load_sem.at[sem])
        copy.start()
        return copy

    old_load, new_load = load(old_hbm, old, 0), load(new_hbm, new, 1)
    grad_load = load(grad_hbm, grad, 2)
    arrays = ((master_hbm, master), (one_hbm, one), (two_hbm, two))
    def load_layer(layer):
        return [load(src.at[layer], dst[layer], 3 + 3 * layer + i) for i, (src, dst) in enumerate(arrays)]

    loads = [load_layer(0)]

    old_load.wait()
    new_load.wait()
    here = lax.broadcasted_iota(jnp.int32, (GROUP, GROUP * slots), 0)
    diagonal = lax.broadcasted_iota(jnp.int32, (GROUP, GROUP), 0) == lax.broadcasted_iota(
        jnp.int32, (GROUP, GROUP), 1
    )
    for layer in range(layers):
        was, now = old[layer : layer + 1], new[layer : layer + 1]
        word = jnp.where(was != now, (was // slots) * slots + now % slots, 0)
        word = jnp.where(now // slots == here, word, 0)
        word = jnp.sum(word, axis=1, keepdims=True)
        plan_rows[layer : layer + 1] = jnp.sum(jnp.where(diagonal, word, 0), axis=0, keepdims=True)
    plan_copy = pltpu.make_async_copy(plan_rows, plan, load_sem.at[9])
    plan_copy.start()

    grad_load.wait()

    def square(i, accs):
        accs = list(accs)
        for c in range(full):
            g = grad[i // slots, i % slots, :, c * LANES : (c + 1) * LANES].astype(jnp.float32)
            accs[c % CHAINS] += g * g
        return tuple(accs)

    zero = jnp.zeros((rows, LANES), jnp.float32)
    acc = sum(lax.fori_loop(0, layers * slots, square, (zero,) * CHAINS))
    tail = grad[:, :, :, full * LANES :].astype(jnp.float32)
    tail = jnp.sum((tail * tail).reshape(layers * slots * rows, cols - full * LANES), axis=0, keepdims=True)
    acc = jnp.sum(acc, axis=0, keepdims=True)
    part[...] = acc + jnp.concatenate([tail, jnp.zeros_like(tail)], axis=1)
    parts[pl.ds(me, 1)] = part[...].reshape(1, 1, LANES)

    loads.append(load_layer(1))
    pl.semaphore_wait(barrier, len(MOVES) + DP - 1)

    for t in targets:
        pltpu.make_async_remote_copy(
            part, parts.at[me], part_sem.at[0], part_sem.at[1], device_id={"expert": t}
        ).start()

    for copy in loads[0]:
        copy.wait()
    plan_copy.wait()

    my_move = [plan[layer, me] % slots for layer in range(layers)]

    def units(x):
        return x.reshape(rows // SUB, SUB, LANES)

    def joined(x):
        x = x.reshape(rows // SUB // 2, 2, SUB, cols - full * LANES)
        return jnp.concatenate([x[:, 0], x[:, 1]], axis=-1)

    for i, ref in enumerate((master_0, one_0, two_0, grad.at[0])):
        for c in range(full):
            x = ref[my_move[0], :, c * LANES : (c + 1) * LANES].astype(jnp.float32)
            send_raw[4 * c : 4 * c + 4, i] = units(x)
        x = ref[my_move[0], :, full * LANES :].astype(jnp.float32)
        send_raw[4 * full : 4 * full + 2, i] = joined(x)

    def bytes_of(ref, sem):
        return pltpu.make_async_copy(ref, ref, sem)

    def sized(layer, holder, body):
        short = is_short(layer, holder)

        @pl.when(short)
        def _():
            body(PIECE - 1)

        @pl.when(jnp.logical_not(short))
        def _():
            body(PIECE)

    def post(src, dst, batch, t):
        pltpu.make_async_remote_copy(
            src, dst, out_sem.at[batch, 0], out_sem.at[batch, 1], device_id={"expert": t}
        ).start()

    def out(send, hold, layer, batch):
        for t in targets:

            def start(size):
                src = send.at[pl.ds(offset(layer, t), size)]
                post(src, hold.at[me, pl.ds(0, size)], batch, t)

            sized(layer, t, start)

        def keep(size):
            hold[pl.ds(me, 1), 0:size] = send[pl.ds(offset(layer, me), size)][None]

        sized(layer, me, keep)

    def arrived(hold, layer, batch):
        def wait(size):
            bytes_of(hold.at[0 : GROUP - 1, 0:size], out_sem.at[batch, 1]).wait()

        sized(layer, me, wait)

    def sent(send, layer, batch):
        def wait(size):
            bytes_of(send.at[0 : UNITS - size], out_sem.at[batch, 0]).wait()

        sized(layer, me, wait)

    def reply(src, dst, batch, t):
        pltpu.make_async_remote_copy(
            src, dst, back_sem.at[batch, 0], back_sem.at[batch, 1], device_id={"expert": t}
        ).start()

    def other_whole(body):
        whole = GROUP - sum(is_short(0, holder) for holder in range(GROUP))
        short = is_short(0, me)

        @pl.when(short)
        def _():
            body(whole)

        @pl.when(jnp.logical_not(short))
        def _():
            body(whole - 1)

    for t in near_first:
        post(send_raw.at[pl.ds(offset(0, t), RAW)], hold_raw.at[me], 0, t)
    hold_raw[pl.ds(me, 1)] = send_raw[pl.ds(offset(0, me), RAW)][None]
    for copy in loads[1]:
        copy.wait()

    for c in range(full):
        x = master_1[my_move[1], :, c * LANES : (c + 1) * LANES]
        send_master[4 * c : 4 * c + 4] = units(x)
    send_master[4 * full : 4 * full + 2] = joined(master_1[my_move[1], :, full * LANES :])
    out(send_master, hold_master, 1, 1)

    bytes_of(parts.at[0 : GROUP - 1], part_sem.at[1]).wait()
    line[...] = jnp.sum(parts[...].reshape(GROUP, LANES), axis=0, keepdims=True)
    lines[pl.ds(dp, 1)] = line[...].reshape(1, 1, LANES)
    for d in range(1, DP):
        pltpu.make_async_remote_copy(
            line, lines.at[dp], part_sem.at[2], part_sem.at[3], device_id={"dp": (dp + d) % DP}
        ).start()
    bytes_of(lines.at[0 : DP - 1], part_sem.at[3]).wait()
    total = jnp.sum(lines[...].reshape(DP, LANES), axis=0, keepdims=True)
    total = jnp.sum(total, axis=1, keepdims=True)
    scale = jnp.minimum(1.0, CLIP_RMS * math.sqrt(entry_count) / (jnp.sqrt(total) + 1e-06))

    for holder in range(GROUP):
        if not is_short(0, holder):
            x = send_raw[offset(0, holder) + RAW]
            for i, y in enumerate(adam(x[0], x[1], x[2], x[3], scale)):
                send_rest[holder, i] = y
    for t in targets:

        @pl.when(jnp.logical_not(is_short(0, t)))
        def _():
            post(send_rest.at[t], hold_rest.at[me], 2, t)

    hold_rest[pl.ds(me, 1)] = send_rest[pl.ds(me, 1)]

    def inputs(layer, at):
        return (
            master[layer][at],
            one[layer][at],
            two[layer][at],
            grad[(layer, *at)].astype(jnp.float32),
        )

    for c in range(full):
        at = (my_move[1], slice(None), slice(c * LANES, (c + 1) * LANES))
        for i, x in enumerate(moments(*inputs(1, at)[1:], scale)):
            send_new[4 * c : 4 * c + 4, i] = units(x)
    at = (my_move[1], slice(None), slice(full * LANES, cols))
    for i, x in enumerate(moments(*inputs(1, at)[1:], scale)):
        send_new[4 * full : 4 * full + 2, i] = joined(x)
    out(send_new, hold_new, 1, 3)

    bytes_of(hold_raw.at[0 : GROUP - 1], out_sem.at[0, 1]).wait()

    def forward_raw(t, _):
        source = plan[0, t] // slots
        x = hold_raw[source]
        for i, y in enumerate(adam(x[:, 0], x[:, 1], x[:, 2], x[:, 3], scale)):
            back_0[t, :, i] = y
        return 0

    lax.fori_loop(0, GROUP, forward_raw, 0)
    here = pl.ds(offset(0, me), RAW)
    for t in targets:
        reply(back_0.at[t], home_0.at[here], 0, t)
    home_0[here] = back_0[me]

    @pl.when(jnp.logical_not(is_short(0, me)))
    def _():
        bytes_of(hold_rest.at[0 : GROUP - 1], out_sem.at[2, 1]).wait()

        def forward_rest(t, _):
            back_rest[t] = hold_rest[plan[0, t] // slots]
            return 0

        lax.fori_loop(0, GROUP, forward_rest, 0)
        for t in targets:
            reply(back_rest.at[t], home_0.at[offset(0, me) + RAW], 1, t)
        home_0[pl.ds(offset(0, me) + RAW, 1)] = back_rest[pl.ds(me, 1)]

    arrived(hold_master, 1, 1)
    arrived(hold_new, 1, 3)

    def forward_new(t):
        source = plan[1, t] // slots
        x = hold_new[source]
        back_1[t, :, 0] = stepped(hold_master[source], x[:, 0], x[:, 1])
        back_1[t, :, 1:3] = x

    def send_back(some):
        def start(size):
            for t in some:
                src = back_1.at[t, pl.ds(0, size)]
                reply(src, home_1.at[pl.ds(offset(1, me), size)], 2, t)

        sized(1, me, start)

    groups = [targets[k : k + BATCH] for k in range(0, len(targets), BATCH)]
    for some, before in zip(groups + [[me]], [[]] + groups):
        for t in some:
            forward_new(t)
        send_back(before)

    def keep_back(size):
        home_1[pl.ds(offset(1, me), size)] = back_1[me, 0:size]

    sized(1, me, keep_back)

    for layer in range(layers):

        def resident(slot, _):
            for lo in range(0, cols, 2 * LANES):
                at = (slot, slice(None), slice(lo, min(lo + 2 * LANES, cols)))
                for ref, x in zip((new_w, new_one, new_two), adam(*inputs(layer, at), scale)):
                    ref[(layer, *at)] = x
            return 0

        lax.fori_loop(0, slots, resident, 0)

    bytes_of(home_0.at[0 : RAW * (GROUP - 1)], back_sem.at[0, 1]).wait()
    other_whole(lambda count: bytes_of(home_0.at[0:count], back_sem.at[1, 1]).wait())
    unpack(home_0, landed)
    sized(1, me, lambda size: bytes_of(home_1.at[0 : UNITS - size], back_sem.at[2, 1]).wait())

    bytes_of(parts.at[0 : GROUP - 1], part_sem.at[0]).wait()
    bytes_of(lines.at[0 : DP - 1], part_sem.at[2]).wait()
    bytes_of(send_raw.at[0 : RAW * (GROUP - 1)], out_sem.at[0, 0]).wait()
    sent(send_master, 1, 1)
    other_whole(lambda count: bytes_of(send_rest.at[0:count], out_sem.at[2, 0]).wait())
    sent(send_new, 1, 3)
    bytes_of(back_0.at[0 : GROUP - 1], back_sem.at[0, 0]).wait()

    @pl.when(jnp.logical_not(is_short(0, me)))
    def _():
        bytes_of(back_rest.at[0 : GROUP - 1], back_sem.at[1, 0]).wait()

    sized(
        1, me, lambda size: bytes_of(back_1.at[0 : GROUP - 1, 0:size], back_sem.at[2, 0]).wait()
    )


def exchange(master, moment_one, moment_two, gradient, old_slot, new_slot, entry_count):
    layers, slots, rows, cols = master.shape
    vmem = pl.BlockSpec(memory_space=pltpu.VMEM)
    f32 = jnp.float32
    dma = pltpu.SemaphoreType.DMA
    return pl.pallas_call(
        functools.partial(exchange_kernel, entry_count),
        out_shape=[jax.ShapeDtypeStruct(master.shape, f32)] * 3
        + [
            jax.ShapeDtypeStruct((3, rows, cols), f32),
            jax.ShapeDtypeStruct((UNITS, 3, SUB, LANES), f32),
            jax.ShapeDtypeStruct((layers, GROUP), jnp.int32),
        ],
        in_specs=[pl.BlockSpec(memory_space=pltpu.HBM)] * 6,
        out_specs=[vmem] * 6,
        scratch_shapes=[
            pltpu.VMEM(old_slot.shape, jnp.int32),
            pltpu.VMEM(new_slot.shape, jnp.int32),
            pltpu.SMEM((layers, GROUP), jnp.int32),
            *[pltpu.VMEM(master.shape[1:], f32)] * (3 * layers),
            pltpu.VMEM(master.shape, jnp.bfloat16),
            pltpu.VMEM((UNITS, 4, SUB, LANES), f32),
            pltpu.VMEM((UNITS, SUB, LANES), f32),
            pltpu.VMEM((GROUP, 3, SUB, LANES), f32),
            pltpu.VMEM((UNITS, 2, SUB, LANES), f32),
            pltpu.VMEM((GROUP, RAW, 4, SUB, LANES), f32),
            pltpu.VMEM((GROUP, PIECE, SUB, LANES), f32),
            pltpu.VMEM((GROUP, 3, SUB, LANES), f32),
            pltpu.VMEM((GROUP, PIECE, 2, SUB, LANES), f32),
            pltpu.VMEM((GROUP, RAW, 3, SUB, LANES), f32),
            pltpu.VMEM((GROUP, 3, SUB, LANES), f32),
            pltpu.VMEM((GROUP, PIECE, 3, SUB, LANES), f32),
            pltpu.VMEM((UNITS, 3, SUB, LANES), f32),
            pltpu.VMEM((1, LANES), f32),
            pltpu.VMEM((GROUP, 1, LANES), f32),
            pltpu.VMEM((1, LANES), f32),
            pltpu.VMEM((DP, 1, LANES), f32),
            dma((10,)),
            dma((4,)),
            dma((4, 2)),
            dma((3, 2)),
        ],
        compiler_params=pltpu.CompilerParams(
            collective_id=0, has_side_effects=True, vmem_limit_bytes=40 * 1024 * 1024
        ),
        name="exchange",
    )(
        *(
            pltpu.with_memory_space_constraint(x, pltpu.HBM)
            for x in (master, moment_one, moment_two, gradient, old_slot, new_slot)
        )
    )


def place_kernel(plan, w, one, two, landed, home, out_w, out_one, out_two, last, sem):
    layers, slots = w.shape[:2]
    pairs = ((w, out_w), (one, out_one), (two, out_two))
    mine = lax.broadcasted_iota(jnp.int32, plan.shape, 1) == lax.axis_index("expert")
    chosen = jnp.where(mine, plan[...], 0)
    moved = [jnp.sum(chosen[layer : layer + 1]) % slots for layer in range(layers)]
    for layer in range(layers):
        for i, (src, dst) in enumerate(pairs):
            for slot in range(slots):

                @pl.when(slot != moved[layer])
                def _():
                    pltpu.make_async_copy(
                        src.at[layer, slot], dst.at[layer, slot], sem.at[i]
                    ).start()

    unpack(home, last)
    for layer, block in enumerate((landed, last)):
        for i, (_, dst) in enumerate(pairs):
            pltpu.make_async_copy(block.at[i], dst.at[layer, moved[layer]], sem.at[i]).start()
    for i, (src, dst) in enumerate(pairs):
        pltpu.make_async_copy(src, dst, sem.at[i]).wait()


def place(plan, w, one, two, landed, home):
    rows, cols = w.shape[2:]
    vmem = pl.BlockSpec(memory_space=pltpu.VMEM)
    free = pl.BlockSpec(memory_space=pl.ANY)
    return pl.pallas_call(
        place_kernel,
        out_shape=[jax.ShapeDtypeStruct(w.shape, w.dtype)] * 3,
        in_specs=[vmem] + [free] * 4 + [vmem],
        out_specs=[free] * 3,
        scratch_shapes=[pltpu.VMEM((3, rows, cols), w.dtype), pltpu.SemaphoreType.DMA((3,))],
        compiler_params=pltpu.CompilerParams(vmem_limit_bytes=4 * 1024 * 1024),
        name="place",
    )(plan, w, one, two, landed, home)


def shards(master, moment_one, moment_two, gradient, old_slot, new_slot):
    layers, slots, rows, cols = master.shape
    entry_count = layers * slots * GROUP * rows * DP * cols
    w, one, two, landed, home, plan = exchange(
        master, moment_one, moment_two, gradient, old_slot, new_slot, entry_count
    )
    return place(plan, w, one, two, landed, home)


def solution(mesh):
    spec = P(None, "expert", "dp", None)
    return jax.shard_map(
        shards,
        mesh=mesh,
        in_specs=(spec, spec, spec, spec, P(), P()),
        out_specs=(spec, spec, spec),
        check_vma=False,
    )
```
